128 devices in a mesh: row: 16 (over z_hi, y, core), col: 8 (over x, z_lo).
Axes of the slice: x: 4, y: 4, z: 4 (z_hi: 2, z_lo: 2; z = z_hi * 2 + z_lo), core: 2. Of those that a mesh axis runs over, the one named last changes fastest.
Arguments:
- alignment_tensor: bfloat16 [128, 1024, 256], P(None, ('row', 'col')), may hold values from -6 to 6
- alignment_scaling_vector: float32 [256], replicated, may hold values from 0.1 to 1.9
- first_factor_matrix: bfloat16 [256, 32], replicated, may hold values from -0.375 to 0.375
- second_factor_matrix: bfloat16 [256, 32], replicated, may hold values from -0.375 to 0.375
- final_mapping_matrix: bfloat16 [1024, 128], replicated, may hold values from -2 to 2
- final_offset_vector: float32 [128], replicated, may hold values from -3 to 3
- couple_tensor: bfloat16 [1024, 1024, 128], P('row', 'col'), may hold values from -6 to 6
- feedforward_scaling_vector: float32 [128], replicated, may hold values from 0.1 to 1.9
- feedforward_expand_matrix: bfloat16 [128, 512], replicated, may hold values from -0.5 to 0.5
- feedforward_contract_matrix: bfloat16 [512, 128], replicated, may hold values from -0.25 to 0.25
- upstream_sensitivity: bfloat16 [1024, 1024, 128], P('row', 'col'), may hold values from -6 to 6
Outputs:
- couple_revised_tensor: bfloat16 [1024, 1024, 128], P('row', 'col')
- couple_sensitivity: bfloat16 [1024, 1024, 128], P('row', 'col')
- alignment_sensitivity: bfloat16 [128, 1024, 256], P(None, ('row', 'col'))
- grad_out_proj: float32 [1024, 128], replicated
- grad_trans_in: float32 [128, 512], replicated
- grad_trans_out: float32 [512, 128], replicated
- first_factor_matrix_sensitivity: float32 [256, 32], replicated
- second_factor_matrix_sensitivity: float32 [256, 32], replicated
The draws below stay inside these ranges and needn't reach their ends.
All inputs are finite; a program needn't handle non-finite values.
Results may differ from the reference program's by a relative error of at most 0.02.
Values may be sent and summed in bfloat16 or wider, within the bound.
No kernel may reach another device: no remote copies, remote signals or barrier semaphores. Data moves between devices by JAX's collectives and lax.ppermute only.
A program may use at most 64 MiB of HBM per device.

```python
import jax
import jax.numpy as jnp
from jax import lax

ALIGN_FEATURES = 256
SIDE_DIM = 32
CZ = 128
TRANS_WIDTH = 512
ALIGNED_NUMBER = 128
AMINO_NUMBER = 1024


def block_scale(own_key, shape, cuts, smallest, largest):
    level, own = 1.0, jax.random.fold_in(own_key, 6)
    for position, parts in cuts:
        draws = jnp.exp(jax.random.uniform(jax.random.fold_in(own, position), (parts,), jnp.float32, smallest / len(cuts), largest / len(cuts)))
        level = level * jnp.repeat(draws, shape[position] // parts).reshape([-1 if axis == position else 1 for axis in range(len(shape))])
    return level


def gaussian(stream_key, dims, deviation, bound, shards=(), kind=jnp.bfloat16):
    values = deviation * jax.random.normal(stream_key, dims, jnp.float32)
    if shards:
        values = values * block_scale(stream_key, dims, shards, -0.22, 0.18)
    return jnp.clip(values, -bound, bound).astype(kind)


def setup_inputs(seed: int = 0) -> dict:
    key_of = jax.random.split(jax.random.key(seed), 12)
    alignment_tensor = gaussian(key_of[0], (ALIGNED_NUMBER, AMINO_NUMBER, ALIGN_FEATURES), 1.0, 6.0, ((1, 128),))
    alignment_scaling_vector = jnp.clip(1.0 + 0.18 * jax.random.normal(key_of[1], (ALIGN_FEATURES,), jnp.float32), 0.1, 1.9)
    first_factor_matrix = gaussian(key_of[2], (ALIGN_FEATURES, SIDE_DIM), ALIGN_FEATURES ** -0.5, 0.375)
    second_factor_matrix = gaussian(key_of[3], (ALIGN_FEATURES, SIDE_DIM), ALIGN_FEATURES ** -0.5, 0.375)
    final_mapping_matrix = gaussian(key_of[4], (SIDE_DIM * SIDE_DIM, CZ), (SIDE_DIM * SIDE_DIM // ALIGNED_NUMBER) ** -0.5, 2.0)
    final_offset_vector = gaussian(key_of[5], (CZ,), 0.5, 3.0, (), jnp.float32)
    couple_tensor = gaussian(key_of[6], (AMINO_NUMBER, AMINO_NUMBER, CZ), 1.0, 6.0, ((0, 16), (1, 8)))
    feedforward_scaling_vector = jnp.clip(1.0 + 0.18 * jax.random.normal(key_of[7], (CZ,), jnp.float32), 0.1, 1.9)
    feedforward_expand_matrix = gaussian(key_of[8], (CZ, TRANS_WIDTH), CZ ** -0.5, 0.5)
    feedforward_contract_matrix = gaussian(key_of[9], (TRANS_WIDTH, CZ), TRANS_WIDTH ** -0.5, 0.25)
    upstream_sensitivity = gaussian(key_of[10], (AMINO_NUMBER, AMINO_NUMBER, CZ), 1.0, 6.0, ((0, 16), (1, 8)))
    return dict(alignment_tensor=alignment_tensor, alignment_scaling_vector=alignment_scaling_vector, first_factor_matrix=first_factor_matrix, second_factor_matrix=second_factor_matrix, final_mapping_matrix=final_mapping_matrix, final_offset_vector=final_offset_vector, couple_tensor=couple_tensor, feedforward_scaling_vector=feedforward_scaling_vector, feedforward_expand_matrix=feedforward_expand_matrix, feedforward_contract_matrix=feedforward_contract_matrix, upstream_sensitivity=upstream_sensitivity)


EPSILON = 1e-05
ROOT_HALF = 0.7071067811865476
INV_ROOT_TWO_PI = 0.3989422804014327

def smooth_gate(values):
    return 0.5 * values * (1.0 + jax.scipy.special.erf(values * ROOT_HALF))

def smooth_slope(values):
    return 0.5 * (1.0 + jax.scipy.special.erf(values * ROOT_HALF)) + values * jnp.exp(-0.5 * values * values) * INV_ROOT_TWO_PI

def standardize_features(values, gain_vec):
    average = lax.optimization_barrier(jnp.mean(values, axis=-1, keepdims=True))
    centred = values - average
    variance = lax.optimization_barrier(jnp.mean(centred * centred, axis=-1, keepdims=True))
    inv_scale = lax.rsqrt(variance + EPSILON)
    vhat_values = centred * inv_scale
    return (vhat_values * gain_vec, vhat_values, inv_scale)

def standardize_reverse_mode(incoming, vhat_values, inv_scale, gain_vec):
    scaled = incoming * gain_vec
    return inv_scale * (scaled - lax.optimization_barrier(jnp.mean(scaled, axis=-1, keepdims=True)) - vhat_values * lax.optimization_barrier(jnp.mean(scaled * vhat_values, axis=-1, keepdims=True)))

def reference(alignment_tensor, alignment_scaling_vector, first_factor_matrix, second_factor_matrix, final_mapping_matrix, final_offset_vector, couple_tensor, feedforward_scaling_vector, feedforward_expand_matrix, feedforward_contract_matrix, upstream_sensitivity):
    aligned_number, amino_number, alignment_feature_size = alignment_tensor.shape
    channels = first_factor_matrix.shape[1]
    pair_width = couple_tensor.shape[2]
    rescaled_complete_lines, alignment_centered_scaled, alignment_reciprocal_spread = standardize_features(alignment_tensor.astype(jnp.float32), alignment_scaling_vector.astype(jnp.float32))
    rescaled_lines = rescaled_complete_lines.astype(jnp.bfloat16)
    alignment_matrix_lines = rescaled_lines.reshape(aligned_number * amino_number, alignment_feature_size)
    first_factor_values = jnp.dot(alignment_matrix_lines, first_factor_matrix, preferred_element_type=jnp.float32).astype(jnp.bfloat16)
    second_factor_values = jnp.dot(alignment_matrix_lines, second_factor_matrix, preferred_element_type=jnp.float32).astype(jnp.bfloat16)
    left_full = first_factor_values.astype(jnp.float32).reshape(aligned_number, amino_number, channels)
    right_full = second_factor_values.astype(jnp.float32).reshape(aligned_number, amino_number, channels)
    block_rows = 64 if amino_number % 64 == 0 else amino_number
    gain_pair = feedforward_scaling_vector.astype(jnp.float32)

    def block_step(totals, start_row):
        acc_right, summed_result_state, summed_entry_state, summed_feedforward_result = totals
        left_block = lax.dynamic_slice_in_dim(left_full, start_row, block_rows, 1)
        outer_prod = (jnp.einsum('sic,sje->ijce', left_block, right_full) / aligned_number).astype(jnp.bfloat16)
        outer_prod = outer_prod.reshape(block_rows * amino_number, channels * channels)
        pair_block = lax.dynamic_slice_in_dim(couple_tensor, start_row, block_rows, 0).reshape(-1, pair_width)
        cot_block = lax.dynamic_slice_in_dim(upstream_sensitivity, start_row, block_rows, 0).reshape(-1, pair_width)
        update = jnp.dot(outer_prod, final_mapping_matrix, preferred_element_type=jnp.float32) + final_offset_vector.astype(jnp.float32)
        middle = (pair_block.astype(jnp.float32) + update).astype(jnp.bfloat16)
        middle_full = middle.astype(jnp.float32)
        normed_pair_full, pair_hat, pair_inv = standardize_features(middle_full, gain_pair)
        normed_pair = normed_pair_full.astype(jnp.bfloat16)
        pre_gate = jnp.dot(normed_pair, feedforward_expand_matrix, preferred_element_type=jnp.float32)
        hidden = smooth_gate(pre_gate).astype(jnp.bfloat16)
        result = (middle_full + jnp.dot(hidden, feedforward_contract_matrix, preferred_element_type=jnp.float32)).astype(jnp.bfloat16)
        cot_full = cot_block.astype(jnp.float32)
        summed_feedforward_result = summed_feedforward_result + jnp.einsum('pk,pn->kn', hidden.astype(jnp.float32), cot_full)
        hidden_grad = (jnp.dot(cot_block, feedforward_contract_matrix.T, preferred_element_type=jnp.float32) * smooth_slope(pre_gate)).astype(jnp.bfloat16)
        summed_entry_state = summed_entry_state + jnp.einsum('pk,pn->kn', normed_pair.astype(jnp.float32), hidden_grad.astype(jnp.float32))
        norm_grad = jnp.dot(hidden_grad, feedforward_expand_matrix.T, preferred_element_type=jnp.float32)
        grad_block = (cot_full + standardize_reverse_mode(norm_grad, pair_hat, pair_inv, gain_pair)).astype(jnp.bfloat16)
        summed_result_state = summed_result_state + jnp.einsum('pk,pn->kn', outer_prod.astype(jnp.float32), grad_block.astype(jnp.float32))
        outer_grad = jnp.dot(grad_block, final_mapping_matrix.T, preferred_element_type=jnp.float32).astype(jnp.bfloat16)
        outer_grad = outer_grad.astype(jnp.float32).reshape(block_rows, amino_number, channels, channels)
        left_part = jnp.einsum('ijce,sje->sic', outer_grad, right_full) / aligned_number
        acc_right = acc_right + jnp.einsum('ijce,sic->sje', outer_grad, left_block) / aligned_number
        return ((acc_right, summed_result_state, summed_entry_state, summed_feedforward_result), (result.reshape(block_rows, amino_number, pair_width), grad_block.reshape(block_rows, amino_number, pair_width), left_part))
    initial = (jnp.zeros((aligned_number, amino_number, channels), jnp.float32), jnp.zeros((channels * channels, pair_width), jnp.float32), jnp.zeros(feedforward_expand_matrix.shape, jnp.float32), jnp.zeros(feedforward_contract_matrix.shape, jnp.float32))
    starts = jnp.arange(amino_number // block_rows, dtype=jnp.int32) * block_rows
    totals, stacked = lax.scan(block_step, initial, starts)
    acc_right, summed_result_state, summed_entry_state, summed_feedforward_result = totals
    results, grad_blocks, left_parts = stacked
    couple_revised_tensor = results.reshape(amino_number, amino_number, pair_width)
    couple_sensitivity = grad_blocks.reshape(amino_number, amino_number, pair_width)
    left_grad = jnp.moveaxis(left_parts, 0, 1).reshape(aligned_number, amino_number, channels).astype(jnp.bfloat16)
    right_grad = acc_right.astype(jnp.bfloat16)
    left_flat = left_grad.reshape(aligned_number * amino_number, channels)
    right_flat = right_grad.reshape(aligned_number * amino_number, channels)
    rescaled_broad_lines = alignment_matrix_lines.astype(jnp.float32)
    first_factor_matrix_sensitivity = jnp.einsum('pm,pc->mc', rescaled_broad_lines, left_flat.astype(jnp.float32)) / amino_number
    second_factor_matrix_sensitivity = jnp.einsum('pm,pc->mc', rescaled_broad_lines, right_flat.astype(jnp.float32)) / amino_number
    rescaled_sensitivity = jnp.dot(left_flat, first_factor_matrix.T, preferred_element_type=jnp.float32) + jnp.dot(right_flat, second_factor_matrix.T, preferred_element_type=jnp.float32)
    rescaled_sensitivity = rescaled_sensitivity.reshape(aligned_number, amino_number, alignment_feature_size)
    alignment_sensitivity = standardize_reverse_mode(rescaled_sensitivity, alignment_centered_scaled, alignment_reciprocal_spread, alignment_scaling_vector.astype(jnp.float32)).astype(jnp.bfloat16)
    return (couple_revised_tensor, couple_sensitivity, alignment_sensitivity, summed_result_state / amino_number, summed_entry_state / amino_number, summed_feedforward_result / amino_number, first_factor_matrix_sensitivity, second_factor_matrix_sensitivity)
```

```python
import jax
import jax.numpy as jnp
from jax import lax
from jax.experimental import pallas as pl
from jax.experimental.pallas import tpu as pltpu
from jax.sharding import PartitionSpec as P

EPSILON = 1e-05
ROOT_HALF = 0.7071067811865476
INV_ROOT_TWO_PI = 0.3989422804014327

F32 = jnp.float32
BF16 = jnp.bfloat16
BOTH = ("row", "col")


def matmul(a, b):
    return lax.dot_general(a, b, (((1,), (0,)), ((), ())), preferred_element_type=F32)


def matmul_nt(a, b):
    return lax.dot_general(a, b, (((1,), (1,)), ((), ())), preferred_element_type=F32)


def standardize_features(values, gain_vec):
    average = jnp.mean(values, axis=-1, keepdims=True)
    centred = values - average
    variance = jnp.mean(centred * centred, axis=-1, keepdims=True)
    inv_scale = lax.rsqrt(variance + EPSILON)
    vhat_values = centred * inv_scale
    return (vhat_values * gain_vec, vhat_values, inv_scale)


def standardize_reverse_mode(incoming, vhat_values, inv_scale, gain_vec):
    scaled = incoming * gain_vec
    return inv_scale * (
        scaled
        - jnp.mean(scaled, axis=-1, keepdims=True)
        - vhat_values * jnp.mean(scaled * vhat_values, axis=-1, keepdims=True)
    )


def pair_kernel(
    left_ref,
    right_t_ref,
    pair_ref,
    cot_ref,
    proj_ref,
    proj_t_ref,
    expand_ref,
    expand_t_ref,
    contract_ref,
    contract_t_ref,
    offset_ref,
    gain_ref,
    result_ref,
    grad_ref,
    d_left_ref,
    d_right_ref,
    g_proj_ref,
    g_expand_ref,
    g_contract_ref,
    right_scr,
    outer_scr,
    d_outer_scr,
    acc_right,
):
    step = pl.program_id(0)
    rows, seqs = left_ref.shape
    wide = right_t_ref.shape[0]
    width = proj_t_ref.shape[0]
    lanes = pair_ref.shape[1]
    channels = wide // lanes
    block = pair_ref.shape[0]

    @pl.when(step == 0)
    def _():
        for e in range(channels):
            at = slice(e * lanes, (e + 1) * lanes)
            right_scr[:, at] = right_t_ref[at, :].T
        acc_right[...] = jnp.zeros_like(acc_right)
        g_proj_ref[...] = jnp.zeros_like(g_proj_ref)
        g_expand_ref[...] = jnp.zeros_like(g_expand_ref)
        g_contract_ref[...] = jnp.zeros_like(g_contract_ref)

    left = left_ref[...]
    chunk = 2 * lanes
    for t in range(wide // chunk):
        at = slice(t * chunk, (t + 1) * chunk)
        outer_scr[:, at] = matmul(left, right_scr[:, at]).astype(BF16)

    gain = gain_ref[...]
    offset = offset_ref[...]

    def columns(scr, i):
        start = pl.multiple_of(i * channels, channels)
        tiles = [
            scr[pl.ds(start, channels), e * lanes : (e + 1) * lanes] for e in range(channels)
        ]
        return jnp.concatenate(tiles, axis=0)

    def beside(ref, i):
        return jnp.concatenate([ref[i].T, ref[i + 1].T], axis=1)

    def two_rows(p, carry):
        i = 2 * p
        outer = jnp.concatenate([columns(outer_scr, i), columns(outer_scr, i + 1)], axis=1)
        update = matmul(proj_t_ref[...], outer) + offset
        middle = (beside(pair_ref, i).astype(F32) + update).astype(BF16).astype(F32)
        average = jnp.sum(middle, axis=0, keepdims=True) * (1.0 / width)
        centred = middle - average
        variance = jnp.sum(centred * centred, axis=0, keepdims=True) * (1.0 / width)
        inv = lax.rsqrt(variance + EPSILON)
        vhat = centred * inv
        normed = (vhat * gain).astype(BF16)
        pre = matmul(expand_t_ref[...], normed)
        half = 0.5 * (1.0 + lax.erf(pre * ROOT_HALF))
        hidden = (pre * half).astype(BF16)
        slope = half + pre * jnp.exp(-0.5 * pre * pre) * INV_ROOT_TWO_PI
        result = (middle + matmul(contract_t_ref[...], hidden)).astype(BF16)
        result_ref[i] = result[:, :lanes].T
        result_ref[i + 1] = result[:, lanes:].T
        cot = beside(cot_ref, i)
        d_hidden = (matmul(contract_ref[...], cot) * slope).astype(BF16)
        g_contract_ref[...] += matmul_nt(hidden, cot)
        g_expand_ref[...] += matmul_nt(d_hidden, normed)
        q = matmul(expand_ref[...], d_hidden) * gain
        q_mean = jnp.sum(q, axis=0, keepdims=True) * (1.0 / width)
        q_hat = jnp.sum(q * vhat, axis=0, keepdims=True) * (1.0 / width)
        grad = (cot.astype(F32) + inv * (q - q_mean - vhat * q_hat)).astype(BF16)
        grad_ref[i] = grad[:, :lanes].T
        grad_ref[i + 1] = grad[:, lanes:].T
        g_proj_ref[...] += matmul_nt(outer, grad)
        d_outer = matmul(proj_ref[...], grad).astype(BF16)
        for k in range(2):
            start = pl.multiple_of((i + k) * channels, channels)
            for e in range(channels):
                d_outer_scr[pl.ds(start, channels), e * lanes : (e + 1) * lanes] = d_outer[
                    e * channels : (e + 1) * channels, k * lanes : (k + 1) * lanes
                ]
        return carry

    lax.fori_loop(0, block // 2, two_rows, 0)

    d_left_ref[...] = (matmul(d_outer_scr[...], right_t_ref[...]) * (1.0 / seqs)).astype(BF16)
    left_t = left.T
    for t in range(wide // chunk):
        at = slice(t * chunk, (t + 1) * chunk)
        acc_right[:, at] += matmul(left_t, d_outer_scr[:, at])

    @pl.when(step == pl.num_programs(0) - 1)
    def _():
        parts = d_right_ref.shape[0]
        each = d_right_ref.shape[2]
        for e in range(channels):
            tile = acc_right[:, e * lanes : (e + 1) * lanes].T
            d_right_ref[:, e] = tile.reshape(parts, each, seqs).astype(BF16)


def pair_stage(left, right_t, pair, cot, proj, expand, contract, offset, gain, each):
    rows, lanes, width = pair.shape
    seqs = left.shape[1]
    wide = right_t.shape[0]
    channels = wide // lanes
    hidden = expand.shape[1]
    block = 8
    by_e = (
        proj.reshape(channels, channels, width).transpose(1, 0, 2).reshape(channels * channels, width)
    )
    column = lambda v: jnp.broadcast_to(v.astype(F32)[:, None], (width, 2 * lanes))
    whole = lambda shape: pl.BlockSpec(shape, lambda b: (0,) * len(shape))
    tiles = pl.BlockSpec((block, lanes, width), lambda b: (b, 0, 0))
    flat = pl.BlockSpec((block * channels, seqs), lambda b: (b, 0))
    out = pl.pallas_call(
        pair_kernel,
        grid=(rows // block,),
        in_specs=[
            flat,
            whole((wide, seqs)),
            tiles,
            tiles,
            whole((channels * channels, width)),
            whole((width, channels * channels)),
            whole((width, hidden)),
            whole((hidden, width)),
            whole((hidden, width)),
            whole((width, hidden)),
            whole((width, 2 * lanes)),
            whole((width, 2 * lanes)),
        ],
        out_specs=[
            tiles,
            tiles,
            flat,
            whole((lanes // each, channels, each, seqs)),
            whole((channels * channels, width)),
            whole((hidden, width)),
            whole((hidden, width)),
        ],
        out_shape=[
            jax.ShapeDtypeStruct((rows, lanes, width), BF16),
            jax.ShapeDtypeStruct((rows, lanes, width), BF16),
            jax.ShapeDtypeStruct((rows * channels, seqs), BF16),
            jax.ShapeDtypeStruct((lanes // each, channels, each, seqs), BF16),
            jax.ShapeDtypeStruct((channels * channels, width), F32),
            jax.ShapeDtypeStruct((hidden, width), F32),
            jax.ShapeDtypeStruct((hidden, width), F32),
        ],
        scratch_shapes=[
            pltpu.VMEM((seqs, wide), BF16),
            pltpu.VMEM((block * channels, wide), BF16),
            pltpu.VMEM((block * channels, wide), BF16),
            pltpu.VMEM((seqs, wide), F32),
        ],
        compiler_params=pltpu.CompilerParams(
            dimension_semantics=("arbitrary",), vmem_limit_bytes=56 * 1024 * 1024
        ),
        name="pair_stage",
    )(
        left,
        right_t,
        pair,
        cot,
        by_e,
        by_e.T,
        expand,
        expand.T,
        contract,
        contract.T,
        column(offset),
        column(gain),
    )
    result, grad, d_left, d_right, g_proj, g_expand, g_contract = out
    return result, grad, d_left, d_right, g_proj, g_expand, g_contract


def spread(x, axis):
    count = lax.axis_size(axis)
    return lax.all_to_all(
        jnp.broadcast_to(x[None], (count, *x.shape)), axis, 0, 0, tiled=True
    )


def exchange(x, axis):
    return lax.all_to_all(x, axis, 0, 0, tiled=True)


def swap_pairs(rows, cols):
    ratio = rows // cols
    return [
        (r * cols + c, (c * ratio + r % ratio) * cols + r // ratio)
        for r in range(rows)
        for c in range(cols)
    ]


def on_device(
    alignment_tensor,
    alignment_scaling_vector,
    first_factor_matrix,
    second_factor_matrix,
    final_mapping_matrix,
    final_offset_vector,
    couple_tensor,
    feedforward_scaling_vector,
    feedforward_expand_matrix,
    feedforward_contract_matrix,
    upstream_sensitivity,
):
    aligned_number, shard_extent, features = alignment_tensor.shape
    channels = first_factor_matrix.shape[1]
    row_count, col_count, pair_width = couple_tensor.shape
    rows, cols = lax.axis_size("row"), lax.axis_size("col")
    ratio = rows // cols
    amino_number = row_count * rows
    normed_full, msa_hat, msa_inv = standardize_features(
        alignment_tensor.astype(F32), alignment_scaling_vector
    )
    normed = normed_full.astype(BF16)
    left_local = jnp.einsum(
        "srm,mc->rcs", normed, first_factor_matrix, preferred_element_type=F32
    ).astype(BF16)
    right_local = jnp.einsum(
        "srm,me->ers", normed, second_factor_matrix, preferred_element_type=F32
    ).astype(BF16)
    pairs = swap_pairs(rows, cols)
    right_moved = lax.ppermute(right_local, BOTH, pairs)
    left_rows = spread(left_local * (1.0 / aligned_number), "col").reshape(
        row_count * channels, aligned_number
    )
    right_blocks = spread(right_moved, "row")
    right_t = (
        right_blocks.reshape(cols, ratio, channels, shard_extent, aligned_number)
        .transpose(2, 1, 0, 3, 4)
        .reshape(channels * col_count, aligned_number)
    )
    result, grad, d_left, d_right, g_proj, g_expand, g_contract = pair_stage(
        left_rows,
        right_t,
        couple_tensor,
        upstream_sensitivity,
        final_mapping_matrix,
        feedforward_expand_matrix,
        feedforward_contract_matrix,
        final_offset_vector,
        feedforward_scaling_vector,
        shard_extent,
    )
    d_right = (
        d_right.reshape(ratio, cols, channels, shard_extent, aligned_number)
        .transpose(1, 0, 2, 3, 4)
        .reshape(rows, channels, shard_extent, aligned_number)
    )
    d_right = jnp.sum(exchange(d_right, "row").astype(F32), axis=0)
    d_right = lax.ppermute(d_right.astype(BF16), BOTH, pairs)
    d_left = d_left.reshape(cols, shard_extent, channels, aligned_number)
    d_left = jnp.sum(exchange(d_left, "col").astype(F32), axis=0).astype(BF16)

    left_weight = jnp.einsum("srm,rcs->cm", normed, d_left, preferred_element_type=F32)
    right_weight = jnp.einsum("srm,ers->em", normed, d_right, preferred_element_type=F32)
    d_normed = jnp.einsum("rcs,mc->srm", d_left, first_factor_matrix, preferred_element_type=F32)
    d_normed = d_normed + jnp.einsum(
        "ers,me->srm", d_right, second_factor_matrix, preferred_element_type=F32
    )
    alignment_sensitivity = standardize_reverse_mode(
        d_normed, msa_hat, msa_inv, alignment_scaling_vector
    ).astype(BF16)

    lanes = pair_width
    parts = [
        a.astype(BF16).reshape(-1, lanes)
        for a in (g_proj, g_expand, g_contract, left_weight, right_weight)
    ]
    sizes = [a.shape[0] for a in parts]
    devices = rows * cols
    mine = jnp.concatenate(parts, axis=0).reshape(devices, -1, lanes)
    mine = jnp.sum(exchange(mine, BOTH).astype(F32), axis=0) * (1.0 / amino_number)
    total = spread(mine.astype(BF16), BOTH).reshape(-1, lanes).astype(F32)
    at, outs = 0, []
    for size in sizes:
        outs.append(total[at : at + size])
        at += size
    t_proj, t_expand, t_contract, t_left, t_right = outs
    t_proj = t_proj.reshape(channels, channels, pair_width).transpose(1, 0, 2)
    return (
        result,
        grad,
        alignment_sensitivity,
        t_proj.reshape(channels * channels, pair_width),
        t_expand.T,
        t_contract,
        t_left.reshape(channels, features).T,
        t_right.reshape(channels, features).T,
    )


def solution(mesh):
    return jax.shard_map(
        on_device,
        mesh=mesh,
        in_specs=(
            P(None, ("row", "col"), None),
            P(),
            P(),
            P(),
            P(),
            P(),
            P("row", "col", None),
            P(),
            P(),
            P(),
            P("row", "col", None),
        ),
        out_specs=(
            P("row", "col", None),
            P("row", "col", None),
            P(None, ("row", "col"), None),
            P(),
            P(),
            P(),
            P(),
            P(),
        ),
        check_vma=False,
    )
```

```python
import jax
import jax.numpy as jnp
from jax import lax
from jax.experimental import pallas as pl
from jax.experimental.pallas import tpu as pltpu
from jax.sharding import PartitionSpec as P

EPSILON = 1e-05
ROOT_HALF = 0.7071067811865476
INV_ROOT_TWO_PI = 0.3989422804014327

F32 = jnp.float32
BF16 = jnp.bfloat16
CHUNK = 128
BOTH = ("row", "col")


def matmul(a, b):
    return lax.dot_general(a, b, (((1,), (0,)), ((), ())), preferred_element_type=F32)


def matmul_nt(a, b):
    return lax.dot_general(a, b, (((1,), (1,)), ((), ())), preferred_element_type=F32)


def standardize_features(values, gain_vec):
    average = jnp.mean(values, axis=-1, keepdims=True)
    centred = values - average
    variance = jnp.mean(centred * centred, axis=-1, keepdims=True)
    inv_scale = lax.rsqrt(variance + EPSILON)
    vhat_values = centred * inv_scale
    return (vhat_values * gain_vec, vhat_values, inv_scale)


def standardize_reverse_mode(incoming, vhat_values, inv_scale, gain_vec):
    scaled = incoming * gain_vec
    return inv_scale * (
        scaled
        - jnp.mean(scaled, axis=-1, keepdims=True)
        - vhat_values * jnp.mean(scaled * vhat_values, axis=-1, keepdims=True)
    )


def pair_kernel(
    core_ref,
    left_ref,
    own_ref,
    other_ref,
    pair_ref,
    cot_ref,
    proj_ref,
    proj_t_ref,
    expand_ref,
    expand_t_ref,
    contract_ref,
    contract_t_ref,
    offset_ref,
    gain_ref,
    result_ref,
    grad_ref,
    d_left_ref,
    own_out_ref,
    other_out_ref,
    right_t_scr,
    right_scr,
    outer_scr,
    d_outer_scr,
    acc_right,
    hidden_scr,
    d_hidden_scr,
    acc_left,
    left_t_scr,
    g_proj_ref,
    g_expand_ref,
    g_contract_ref,
):
    step = pl.program_id(0)
    first = core_ref[0] == 0
    block = pair_ref.shape[0]
    seqs = left_ref.shape[1]
    wide = right_t_scr.shape[0]
    width = proj_t_ref.shape[0]
    lanes = pair_ref.shape[1]
    channels = wide // lanes
    rows = block * channels
    blocks = left_ref.shape[0] // rows
    chunk = 2 * lanes
    early = rows - 2 * channels

    def left_rows(b, start, size):
        return left_ref[pl.ds(pl.multiple_of(b * rows + start, 2 * channels), size), :]

    def outer_product(b, start, stop, at):
        outer_scr[start:stop, at] = matmul(left_rows(b, start, stop - start), right_scr[:, at]).astype(BF16)

    def pieces(h):
        each = wide // (4 * chunk)
        return [slice((h * each + k) * chunk, (h * each + k + 1) * chunk) for k in range(each)]

    def backward(b, h):
        at = slice(h * wide // 4, (h + 1) * wide // 4)
        part = matmul(d_outer_scr[:, at], right_t_scr[at, :])
        left_t = left_t_scr[...]
        for to in pieces(h):
            acc_right[:, to] += matmul(left_t, d_outer_scr[:, to])
        if h == 0:
            acc_left[...] = part
        elif h < 3:
            acc_left[...] += part
        else:
            total = (acc_left[...] + part) * (1.0 / seqs)
            d_left_ref[pl.ds(pl.multiple_of(b * rows, rows), rows), :] = total.astype(BF16)

    @pl.when(step == 0)
    def _():
        for e in range(channels):
            at = slice(e * lanes, (e + 1) * lanes)
            own, other = own_ref[:, e], other_ref[:, e]
            both = (jnp.where(first, own, other), jnp.where(first, other, own))
            tile = jnp.stack(both, axis=1).reshape(lanes, seqs)
            right_t_scr[at, :] = tile
            right_scr[:, at] = tile.T
        acc_right[...] = jnp.zeros_like(acc_right)
        d_outer_scr[...] = jnp.zeros_like(d_outer_scr)
        g_proj_ref[...] = jnp.zeros_like(g_proj_ref)
        g_expand_ref[...] = jnp.zeros_like(g_expand_ref)
        g_contract_ref[...] = jnp.zeros_like(g_contract_ref)
        for h in range(4):
            for at in pieces(h):
                outer_product(0, 0, early, at)

    before = jnp.maximum(step - 1, 0)
    after = jnp.minimum(step + 1, blocks - 1)
    left_t_scr[...] = left_rows(before, 0, rows).T

    gain = jnp.broadcast_to(gain_ref[...], (2 * lanes, width)).T
    offset = jnp.broadcast_to(offset_ref[...], (2 * lanes, width)).T

    def columns(scr, i, some):
        row = slice(i * channels, (i + 1) * channels)
        tiles = [
            scr[row, e * lanes : (e + 1) * lanes] for e in range(some.start, some.stop)
        ]
        return jnp.concatenate(tiles, axis=0)

    def beside(ref, i):
        return jnp.concatenate([ref[i].T, ref[i + 1].T], axis=1)

    scale = 1.0 / width

    def forward(p):
        i = 2 * p
        outer = jnp.concatenate([columns(outer_scr, i + k, slice(0, channels)) for k in range(2)], axis=1)
        update = matmul(proj_t_ref[...], outer) + offset
        middle = (beside(pair_ref, i).astype(F32) + update).astype(BF16).astype(F32)
        average = jnp.sum(middle, axis=0, keepdims=True) * scale
        centred = middle - average
        variance = jnp.sum(centred * centred, axis=0, keepdims=True) * scale
        inv = lax.rsqrt(variance + EPSILON)
        vhat = centred * inv
        normed = (vhat * gain).astype(BF16)
        return dict(p=p, middle=middle, vhat=vhat, inv=inv, normed=normed,
                    cot=beside(cot_ref, i))

    def activate(st, h):
        p = st["p"]
        at = slice(h * CHUNK, (h + 1) * CHUNK)
        pre = matmul(expand_t_ref[at, :], st["normed"])
        half = 0.5 + 0.5 * lax.erf(pre * ROOT_HALF)
        hidden_scr[p, at, :] = (pre * half).astype(BF16)
        slope = half + pre * jnp.exp(-0.5 * pre * pre) * INV_ROOT_TWO_PI
        d_hidden_scr[p, at, :] = (matmul(contract_ref[at, :], st["cot"]) * slope).astype(BF16)

    def through(st):
        p, i = st["p"], 2 * st["p"]
        cot, vhat = st["cot"], st["vhat"]
        q = matmul(expand_ref[...], d_hidden_scr[p]) * gain
        result = (st["middle"] + matmul(contract_t_ref[...], hidden_scr[p])).astype(BF16)
        result_ref[i] = result[:, :lanes].T
        result_ref[i + 1] = result[:, lanes:].T
        q_mean = jnp.sum(q, axis=0, keepdims=True) * scale
        q_hat = jnp.sum(q * vhat, axis=0, keepdims=True) * scale
        grad = (cot.astype(F32) + st["inv"] * (q - q_mean - vhat * q_hat)).astype(BF16)
        grad_ref[i] = grad[:, :lanes].T
        grad_ref[i + 1] = grad[:, lanes:].T
        st["grad"] = grad

    def weigh(st, h):
        p, i = st["p"], 2 * st["p"]
        part = proj_ref.shape[0] // 4
        at = slice(h * part, (h + 1) * part)
        d_outer = matmul(proj_ref[at, :], st["grad"]).astype(BF16)
        for k in range(2):
            row = slice((i + k) * channels, (i + k + 1) * channels)
            for e in range(part // channels):
                to = h * (part // channels) + e
                d_outer_scr[row, to * lanes : (to + 1) * lanes] = d_outer[
                    e * channels : (e + 1) * channels, k * lanes : (k + 1) * lanes
                ]
        some = slice(h * part // channels, (h + 1) * part // channels)
        outer = jnp.concatenate(
            [columns(outer_scr, i, some), columns(outer_scr, i + 1, some)], axis=1
        )
        g_proj_ref[at, :] += matmul_nt(outer, st["grad"])
        at = slice(h * CHUNK, (h + 1) * CHUNK)
        g_contract_ref[at, :] += matmul_nt(hidden_scr[p, at, :], st["cot"])
        g_expand_ref[at, :] += matmul_nt(d_hidden_scr[p, at, :], st["normed"])

    last = None
    count = block // 2
    for p in range(count + 1):
        now = forward(p) if p < count else None
        if last is not None:
            through(last)
        for h in range(4):
            if now is not None:
                activate(now, h)
            if last is not None:
                weigh(last, h)
            if p == 0:
                for at in pieces(h):
                    outer_product(step, early, rows, at)
                backward(before, h)
            if p == count:
                for at in pieces(h):
                    outer_product(after, 0, early, at)
        last = now

    @pl.when(step == pl.num_programs(0) - 1)
    def _():
        left_t_scr[...] = left_rows(step, 0, rows).T
        for h in range(4):
            backward(step, h)
        each = own_ref.shape[2]
        halves = own_ref.shape[0]

        def hand_out(at, even, odd):
            own_out_ref[:, at, :] = jnp.where(first, even, odd).astype(BF16)
            other_out_ref[:, at, :] = jnp.where(first, odd, even).astype(BF16)

        for e in range(channels):
            tile = acc_right[:, e * lanes : (e + 1) * lanes].T.reshape(halves, 2, each, seqs)
            hand_out(slice(e * each, (e + 1) * each), tile[:, 0], tile[:, 1])

        def weight_rows(k):
            full = width
            per = full // channels
            if k < channels // per:
                cs = range(k * per, (k + 1) * per)
                return jnp.concatenate(
                    [g_proj_ref[pl.ds(c, channels, stride=channels), :] for c in cs], axis=0
                )
            k -= channels // per
            at = slice(k * full, (k + 1) * full)
            if k < g_expand_ref.shape[0] // full:
                return g_expand_ref[at, :].T
            at = slice(at.start - g_expand_ref.shape[0], at.stop - g_expand_ref.shape[0])
            return g_contract_ref[at, :]

        base = channels * each
        for m in range(halves):
            even, odd = weight_rows(2 * m), weight_rows(2 * m + 1)
            own_out_ref[m, base:, :] = jnp.where(first, even, odd).astype(BF16)
            other_out_ref[m, base:, :] = jnp.where(first, odd, even).astype(BF16)


def pair_stage(core, left, own, other, pair, cot, proj, expand, contract, offset, gain):
    each = own.shape[2]
    rows, lanes, width = pair.shape
    seqs = left.shape[1]
    channels = own.shape[1]
    wide = channels * lanes
    hidden = expand.shape[1]
    block = 8
    by_e = (
        proj.reshape(channels, channels, width).transpose(1, 0, 2).reshape(channels * channels, width)
    )
    whole = lambda shape: pl.BlockSpec(shape, lambda b: (0,) * len(shape))
    weights = channels * channels + 2 * hidden
    parts = (own.shape[0], channels * each + weights // (2 * own.shape[0]), width)
    tiles = pl.BlockSpec((block, lanes, width), lambda b: (b, 0, 0))
    flat = whole((rows * channels, seqs))
    return pl.pallas_call(
        pair_kernel,
        grid=(rows // block,),
        in_specs=[
            pl.BlockSpec(memory_space=pltpu.SMEM),
            flat,
            whole(own.shape),
            whole(own.shape),
            tiles,
            tiles,
            whole((channels * channels, width)),
            whole((width, channels * channels)),
            whole((width, hidden)),
            whole((hidden, width)),
            whole((hidden, width)),
            whole((width, hidden)),
            whole((1, width)),
            whole((1, width)),
        ],
        out_specs=[
            tiles,
            tiles,
            flat,
            whole(parts),
            whole(parts),
        ],
        out_shape=[
            jax.ShapeDtypeStruct((rows, lanes, width), BF16),
            jax.ShapeDtypeStruct((rows, lanes, width), BF16),
            jax.ShapeDtypeStruct((rows * channels, seqs), BF16),
            jax.ShapeDtypeStruct(parts, BF16),
            jax.ShapeDtypeStruct(parts, BF16),
        ],
        scratch_shapes=[
            pltpu.VMEM((wide, seqs), BF16),
            pltpu.VMEM((seqs, wide), BF16),
            pltpu.VMEM((block * channels, wide), BF16),
            pltpu.VMEM((block * channels, wide), BF16),
            pltpu.VMEM((seqs, wide), F32),
            pltpu.VMEM((block // 2, hidden, 2 * lanes), BF16),
            pltpu.VMEM((block // 2, hidden, 2 * lanes), BF16),
            pltpu.VMEM((block * channels, seqs), F32),
            pltpu.VMEM((seqs, block * channels), BF16),
            pltpu.VMEM((channels * channels, width), F32),
            pltpu.VMEM((hidden, width), F32),
            pltpu.VMEM((hidden, width), F32),
        ],
        compiler_params=pltpu.CompilerParams(
            dimension_semantics=("arbitrary",), vmem_limit_bytes=56 * 1024 * 1024
        ),
        name="pair_stage",
    )(
        core,
        left,
        own,
        other,
        pair,
        cot,
        by_e,
        by_e.T,
        expand,
        expand.T,
        contract,
        contract.T,
        offset.astype(F32)[None, :],
        gain.astype(F32)[None, :],
    )


def unpack_kernel(
    core_ref, own_ref, other_ref, scale_ref, proj_ref, expand_ref, contract_ref, left_ref, right_ref
):
    first = core_ref[0] == 0
    size = own_ref.shape[2]
    scale = scale_ref[0]
    halves = own_ref.shape[0] - 1

    def chunk(k):
        own, other = own_ref[1 + k // 2].astype(F32), other_ref[1 + k // 2].astype(F32)
        picked = jnp.where(first, own, other) if k % 2 == 0 else jnp.where(first, other, own)
        return picked * scale

    at = 0
    for k in range(proj_ref.shape[0] // size):
        proj_ref[k * size : (k + 1) * size, :] = chunk(at)
        at += 1
    for k in range(expand_ref.shape[1] // size):
        expand_ref[:, k * size : (k + 1) * size] = chunk(at)
        at += 1
    for k in range(contract_ref.shape[0] // size):
        contract_ref[k * size : (k + 1) * size, :] = chunk(at)
        at += 1
    factors = ((own_ref[0].astype(F32) + other_ref[0].astype(F32)) * scale).T
    channels = left_ref.shape[1]
    for h in range(left_ref.shape[0] // size):
        rows = slice(h * size, (h + 1) * size)
        left_ref[rows, :] = factors[:, 2 * h * channels : (2 * h + 1) * channels]
        right_ref[rows, :] = factors[:, (2 * h + 1) * channels : (2 * h + 2) * channels]


def unpack(core, own, other, scale, shapes):
    smem = pl.BlockSpec(memory_space=pltpu.SMEM)
    vmem = pl.BlockSpec(memory_space=pltpu.VMEM)
    return pl.pallas_call(
        unpack_kernel,
        in_specs=[smem, vmem, vmem, smem],
        out_specs=[vmem] * len(shapes),
        out_shape=[jax.ShapeDtypeStruct(shape, F32) for shape in shapes],
        name="unpack",
    )(core, own, other, jnp.full((1,), scale, F32))


def parity_groups():
    rows = lax.axis_size("row")
    return [list(range(k, rows, 2)) for k in range(2)]


def exchange(x, axis):
    groups = parity_groups() if axis == "row" else None
    return lax.all_to_all(x, axis, 0, 0, tiled=True, axis_index_groups=groups)


def spread(x, axis):
    count = lax.axis_size("row") // 2 if axis == "row" else lax.axis_size(axis)
    return exchange(jnp.broadcast_to(x[None], (count, *x.shape)), axis)


def from_partner(x):
    return lax.ppermute(x, "row", [(k, k ^ 1) for k in range(lax.axis_size("row"))])


def summed(x):
    return jnp.sum(x.astype(F32), axis=0).astype(BF16)


def column_pairs(rows, cols):
    there = [(b, (b % rows) * cols + b // rows) for b in range(rows * cols)]
    return there, [(to, at) for at, to in there]


def on_device(
    alignment_tensor,
    alignment_scaling_vector,
    first_factor_matrix,
    second_factor_matrix,
    final_mapping_matrix,
    final_offset_vector,
    couple_tensor,
    feedforward_scaling_vector,
    feedforward_expand_matrix,
    feedforward_contract_matrix,
    upstream_sensitivity,
):
    aligned_number, shard_extent, features = alignment_tensor.shape
    channels = first_factor_matrix.shape[1]
    row_count, col_count, pair_width = couple_tensor.shape
    rows, cols = lax.axis_size("row"), lax.axis_size("col")
    amino_number = row_count * rows
    normed_full, msa_hat, msa_inv = standardize_features(
        alignment_tensor.astype(F32), alignment_scaling_vector
    )
    normed = normed_full.astype(BF16)
    left_local = jnp.einsum(
        "srm,mc->rcs", normed, first_factor_matrix, preferred_element_type=F32
    ).astype(BF16)
    right_local = jnp.einsum(
        "srm,me->ers", normed, second_factor_matrix, preferred_element_type=F32
    ).astype(BF16)
    there, back = column_pairs(rows, cols)
    right_moved = lax.ppermute(right_local, BOTH, there)
    left_rows = spread(left_local * (1.0 / aligned_number), "col")
    right_moved, left_rows = lax.optimization_barrier((right_moved, left_rows))
    own = spread(right_moved, "row")
    other = from_partner(own)
    core = (lax.axis_index("row") % 2).astype(jnp.int32)[None]
    result, grad, d_left, mine, theirs = pair_stage(
        core,
        left_rows.reshape(row_count * channels, aligned_number),
        own,
        other,
        couple_tensor,
        upstream_sensitivity,
        final_mapping_matrix,
        feedforward_expand_matrix,
        feedforward_contract_matrix,
        final_offset_vector,
        feedforward_scaling_vector,
    )
    lanes = pair_width
    mine = (mine.astype(F32) + from_partner(theirs).astype(F32)).astype(BF16)
    mine = summed(exchange(mine, "row"))
    size = channels * shard_extent
    d_right = mine[:size].reshape(channels, shard_extent, aligned_number)
    with_left = jnp.concatenate(
        [d_left.reshape(cols, size, lanes), mine[size:].reshape(cols, -1, lanes)], axis=1
    )
    d_right, with_left = lax.optimization_barrier((d_right, with_left))
    d_right = lax.ppermute(d_right, BOTH, back)
    with_left = summed(exchange(with_left, "col"))
    d_left = with_left[:size].reshape(shard_extent, channels, aligned_number)
    weights = with_left[size:]

    left_weight = jnp.einsum("srm,rcs->cm", normed, d_left, preferred_element_type=F32)
    right_weight = jnp.einsum("srm,ers->em", normed, d_right, preferred_element_type=F32)
    d_normed = jnp.einsum("rcs,mc->srm", d_left, first_factor_matrix, preferred_element_type=F32)
    d_normed = d_normed + jnp.einsum(
        "ers,me->srm", d_right, second_factor_matrix, preferred_element_type=F32
    )
    alignment_sensitivity = standardize_reverse_mode(
        d_normed, msa_hat, msa_inv, alignment_scaling_vector
    ).astype(BF16)

    factors = jnp.concatenate(
        [
            weight[:, k : k + lanes].astype(BF16)
            for k in range(0, features, lanes)
            for weight in (left_weight, right_weight)
        ],
        axis=0,
    )
    count = factors.shape[0]
    gathered = spread(jnp.concatenate([factors, weights], axis=0), "col")
    factors = summed(gathered[:, :count])
    weights = gathered[:, count:].reshape(-1, lanes)
    gathered = spread(jnp.stack([factors, weights], axis=0), "row")
    half = jnp.concatenate([summed(gathered[:, 0])[None], gathered[:, 1]], axis=0)
    outs = unpack(
        core,
        half,
        from_partner(half),
        1.0 / amino_number,
        (
            final_mapping_matrix.shape,
            feedforward_expand_matrix.shape,
            feedforward_contract_matrix.shape,
            first_factor_matrix.shape,
            second_factor_matrix.shape,
        ),
    )
    return (result, grad, alignment_sensitivity, *outs)


def solution(mesh):
    return jax.shard_map(
        on_device,
        mesh=mesh,
        in_specs=(
            P(None, ("row", "col"), None),
            P(),
            P(),
            P(),
            P(),
            P(),
            P("row", "col", None),
            P(),
            P(),
            P(),
            P("row", "col", None),
        ),
        out_specs=(
            P("row", "col", None),
            P("row", "col", None),
            P(None, ("row", "col"), None),
            P(),
            P(),
            P(),
            P(),
            P(),
        ),
        check_vma=False,
    )
```

```python
import jax
import jax.numpy as jnp
from jax import lax
from jax.experimental import pallas as pl
from jax.experimental.pallas import tpu as pltpu
from jax.sharding import PartitionSpec as P

EPSILON = 1e-05
ROOT_HALF = 0.7071067811865476
INV_ROOT_TWO_PI = 0.3989422804014327

F32 = jnp.float32
BF16 = jnp.bfloat16
CHUNK = 128
BOTH = ("row", "col")


def matmul(a, b):
    return lax.dot_general(a, b, (((1,), (0,)), ((), ())), preferred_element_type=F32)


def matmul_nt(a, b):
    return lax.dot_general(a, b, (((1,), (1,)), ((), ())), preferred_element_type=F32)


def pair_kernel(
    core_ref,
    left_ref,
    own_ref,
    other_ref,
    pair_ref,
    cot_ref,
    proj_ref,
    proj_t_ref,
    expand_ref,
    expand_t_ref,
    contract_ref,
    contract_t_ref,
    offset_ref,
    gain_ref,
    result_ref,
    grad_ref,
    d_left_ref,
    own_out_ref,
    other_out_ref,
    right_t_scr,
    right_scr,
    outer_scr,
    d_outer_scr,
    acc_right,
    hidden_scr,
    d_hidden_scr,
    acc_left,
    left_t_scr,
    g_proj_ref,
    g_expand_ref,
    g_contract_ref,
):
    step = pl.program_id(0)
    first = core_ref[0] == 0
    block = pair_ref.shape[0]
    seqs = left_ref.shape[1]
    wide = right_t_scr.shape[0]
    width = proj_t_ref.shape[0]
    lanes = pair_ref.shape[1]
    channels = wide // lanes
    rows = block * channels
    blocks = left_ref.shape[0] // rows
    chunk = 2 * lanes
    early = rows - 2 * channels

    def left_rows(b, start, size):
        return left_ref[pl.ds(pl.multiple_of(b * rows + start, 2 * channels), size), :]

    def outer_product(b, start, stop, at):
        outer_scr[start:stop, at] = matmul(left_rows(b, start, stop - start), right_scr[:, at]).astype(BF16)

    def pieces(h):
        each = wide // (4 * chunk)
        return [slice((h * each + k) * chunk, (h * each + k + 1) * chunk) for k in range(each)]

    def backward(b, h):
        at = slice(h * wide // 4, (h + 1) * wide // 4)
        part = matmul(d_outer_scr[:, at], right_t_scr[at, :])
        left_t = left_t_scr[...]
        for to in pieces(h):
            acc_right[:, to] += matmul(left_t, d_outer_scr[:, to])
        if h == 0:
            acc_left[...] = part
        elif h < 3:
            acc_left[...] += part
        else:
            total = (acc_left[...] + part) * (1.0 / seqs)
            d_left_ref[b, :rows, :] = total.astype(BF16)

    @pl.when(step == 0)
    def _():
        for e in range(channels):
            at = slice(e * lanes, (e + 1) * lanes)
            own, other = own_ref[:, e], other_ref[:, e]
            both = (jnp.where(first, own, other), jnp.where(first, other, own))
            tile = jnp.stack(both, axis=1).reshape(lanes, seqs)
            right_t_scr[at, :] = tile
            right_scr[:, at] = tile.T
        acc_right[...] = jnp.zeros_like(acc_right)
        d_outer_scr[...] = jnp.zeros_like(d_outer_scr)
        g_proj_ref[...] = jnp.zeros_like(g_proj_ref)
        g_expand_ref[...] = jnp.zeros_like(g_expand_ref)
        g_contract_ref[...] = jnp.zeros_like(g_contract_ref)
        for h in range(4):
            for at in pieces(h):
                outer_product(0, 0, early, at)

    before = jnp.maximum(step - 1, 0)
    after = jnp.minimum(step + 1, blocks - 1)
    left_t_scr[...] = left_rows(before, 0, rows).T

    gain = jnp.broadcast_to(gain_ref[...], (2 * lanes, width)).T
    offset = jnp.broadcast_to(offset_ref[...], (2 * lanes, width)).T

    def columns(scr, i, some):
        row = slice(i * channels, (i + 1) * channels)
        tiles = [
            scr[row, e * lanes : (e + 1) * lanes] for e in range(some.start, some.stop)
        ]
        return jnp.concatenate(tiles, axis=0)

    def beside(ref, i):
        return jnp.concatenate([ref[i].T, ref[i + 1].T], axis=1)

    scale = 1.0 / width

    def forward(p):
        i = 2 * p
        outer = jnp.concatenate([columns(outer_scr, i + k, slice(0, channels)) for k in range(2)], axis=1)
        update = matmul(proj_t_ref[...], outer) + offset
        middle = (beside(pair_ref, i).astype(F32) + update).astype(BF16).astype(F32)
        average = jnp.sum(middle, axis=0, keepdims=True) * scale
        centred = middle - average
        variance = jnp.sum(centred * centred, axis=0, keepdims=True) * scale
        inv = lax.rsqrt(variance + EPSILON)
        vhat = centred * inv
        normed = (vhat * gain).astype(BF16)
        return dict(p=p, middle=middle, vhat=vhat, inv=inv, normed=normed,
                    cot=beside(cot_ref, i))

    def activate(st, h):
        p = st["p"]
        at = slice(h * CHUNK, (h + 1) * CHUNK)
        pre = matmul(expand_t_ref[at, :], st["normed"])
        half = 0.5 + 0.5 * lax.erf(pre * ROOT_HALF)
        hidden_scr[p, at, :] = (pre * half).astype(BF16)
        slope = half + pre * jnp.exp(-0.5 * pre * pre) * INV_ROOT_TWO_PI
        d_hidden_scr[p, at, :] = (matmul(contract_ref[at, :], st["cot"]) * slope).astype(BF16)

    def through(st):
        p, i = st["p"], 2 * st["p"]
        cot, vhat = st["cot"], st["vhat"]
        q = matmul(expand_ref[...], d_hidden_scr[p]) * gain
        result = (st["middle"] + matmul(contract_t_ref[...], hidden_scr[p])).astype(BF16)
        result_ref[i] = result[:, :lanes].T
        result_ref[i + 1] = result[:, lanes:].T
        q_mean = jnp.sum(q, axis=0, keepdims=True) * scale
        q_hat = jnp.sum(q * vhat, axis=0, keepdims=True) * scale
        grad = (cot.astype(F32) + st["inv"] * (q - q_mean - vhat * q_hat)).astype(BF16)
        grad_ref[i] = grad[:, :lanes].T
        grad_ref[i + 1] = grad[:, lanes:].T
        st["grad"] = grad

    def weigh(st, h):
        p, i = st["p"], 2 * st["p"]
        part = proj_ref.shape[0] // 4
        at = slice(h * part, (h + 1) * part)
        d_outer = matmul(proj_ref[at, :], st["grad"]).astype(BF16)
        for k in range(2):
            row = slice((i + k) * channels, (i + k + 1) * channels)
            for e in range(part // channels):
                to = h * (part // channels) + e
                d_outer_scr[row, to * lanes : (to + 1) * lanes] = d_outer[
                    e * channels : (e + 1) * channels, k * lanes : (k + 1) * lanes
                ]
        some = slice(h * part // channels, (h + 1) * part // channels)
        outer = jnp.concatenate(
            [columns(outer_scr, i, some), columns(outer_scr, i + 1, some)], axis=1
        )
        g_proj_ref[at, :] += matmul_nt(outer, st["grad"])
        at = slice(h * CHUNK, (h + 1) * CHUNK)
        g_contract_ref[at, :] += matmul_nt(hidden_scr[p, at, :], st["cot"])
        g_expand_ref[at, :] += matmul_nt(d_hidden_scr[p, at, :], st["normed"])

    last = None
    count = block // 2
    for p in range(count + 1):
        now = forward(p) if p < count else None
        if last is not None:
            through(last)
        for h in range(4):
            if now is not None:
                activate(now, h)
            if last is not None:
                weigh(last, h)
            if p == 0:
                for at in pieces(h):
                    outer_product(step, early, rows, at)
                backward(before, h)
            if p == count:
                for at in pieces(h):
                    outer_product(after, 0, early, at)
        last = now

    @pl.when(step == pl.num_programs(0) - 1)
    def _():
        left_t_scr[...] = left_rows(step, 0, rows).T
        for h in range(4):
            backward(step, h)
        each = own_ref.shape[2]
        halves = own_ref.shape[0]

        def hand_out(at, even, odd):
            own_out_ref[:, at, :] = jnp.where(first, even, odd).astype(BF16)
            other_out_ref[:, at, :] = jnp.where(first, odd, even).astype(BF16)

        for e in range(channels):
            tile = acc_right[:, e * lanes : (e + 1) * lanes].T.reshape(halves, 2, each, seqs)
            hand_out(slice(e * each, (e + 1) * each), tile[:, 0], tile[:, 1])

        def weight_rows(k):
            full = width
            per = full // channels
            if k < channels // per:
                cs = range(k * per, (k + 1) * per)
                return jnp.concatenate(
                    [g_proj_ref[pl.ds(c, channels, stride=channels), :] for c in cs], axis=0
                )
            k -= channels // per
            at = slice(k * full, (k + 1) * full)
            if k < g_expand_ref.shape[0] // full:
                return g_expand_ref[at, :].T
            at = slice(at.start - g_expand_ref.shape[0], at.stop - g_expand_ref.shape[0])
            return g_contract_ref[at, :]

        base = channels * each
        for m in range(halves):
            even, odd = weight_rows(2 * m), weight_rows(2 * m + 1)
            own_out_ref[m, base:, :] = jnp.where(first, even, odd).astype(BF16)
            other_out_ref[m, base:, :] = jnp.where(first, odd, even).astype(BF16)


def pair_stage(core, left, own, other, pair, cot, weights, offset, gain, devices):
    by_e, by_e_t, expand, expand_t, contract, contract_t = weights
    each = own.shape[2]
    rows, lanes, width = pair.shape
    seqs = left.shape[1]
    channels = own.shape[1]
    wide = channels * lanes
    hidden = expand.shape[1]
    block = 8
    whole = lambda shape: pl.BlockSpec(shape, lambda b: (0,) * len(shape))
    grads = channels * channels + 2 * hidden
    d_left = (rows // block, block * channels + grads // devices, seqs)
    parts = (own.shape[0], channels * each + grads // (2 * own.shape[0]), width)
    tiles = pl.BlockSpec((block, lanes, width), lambda b: (b, 0, 0))
    flat = whole((rows * channels, seqs))
    return pl.pallas_call(
        pair_kernel,
        grid=(rows // block,),
        in_specs=[
            pl.BlockSpec(memory_space=pltpu.SMEM),
            flat,
            whole(own.shape),
            whole(own.shape),
            tiles,
            tiles,
            whole((channels * channels, width)),
            whole((width, channels * channels)),
            whole((width, hidden)),
            whole((hidden, width)),
            whole((hidden, width)),
            whole((width, hidden)),
            whole((1, width)),
            whole((1, width)),
        ],
        out_specs=[
            tiles,
            tiles,
            whole(d_left),
            whole(parts),
            whole(parts),
        ],
        out_shape=[
            jax.ShapeDtypeStruct((rows, lanes, width), BF16),
            jax.ShapeDtypeStruct((rows, lanes, width), BF16),
            jax.ShapeDtypeStruct(d_left, BF16),
            jax.ShapeDtypeStruct(parts, BF16),
            jax.ShapeDtypeStruct(parts, BF16),
        ],
        scratch_shapes=[
            pltpu.VMEM((wide, seqs), BF16),
            pltpu.VMEM((seqs, wide), BF16),
            pltpu.VMEM((block * channels, wide), BF16),
            pltpu.VMEM((block * channels, wide), BF16),
            pltpu.VMEM((seqs, wide), F32),
            pltpu.VMEM((block // 2, hidden, 2 * lanes), BF16),
            pltpu.VMEM((block // 2, hidden, 2 * lanes), BF16),
            pltpu.VMEM((block * channels, seqs), F32),
            pltpu.VMEM((seqs, block * channels), BF16),
            pltpu.VMEM((channels * channels, width), F32),
            pltpu.VMEM((hidden, width), F32),
            pltpu.VMEM((hidden, width), F32),
        ],
        compiler_params=pltpu.CompilerParams(
            dimension_semantics=("arbitrary",), vmem_limit_bytes=56 * 1024 * 1024
        ),
        name="pair_stage",
    )(
        core,
        left,
        own,
        other,
        pair,
        cot,
        *weights,
        offset.astype(F32)[None, :],
        gain.astype(F32)[None, :],
    )


def unpack_kernel(
    core_ref, own_ref, other_ref, scale_ref, proj_ref, expand_ref, contract_ref, left_ref, right_ref
):
    first = core_ref[0] == 0
    size = own_ref.shape[2]
    scale = scale_ref[0]
    halves = own_ref.shape[0] - 1

    def chunk(k):
        own, other = own_ref[1 + k // 2].astype(F32), other_ref[1 + k // 2].astype(F32)
        picked = jnp.where(first, own, other) if k % 2 == 0 else jnp.where(first, other, own)
        return picked * scale

    at = 0
    for k in range(proj_ref.shape[0] // size):
        proj_ref[k * size : (k + 1) * size, :] = chunk(at)
        at += 1
    for k in range(expand_ref.shape[1] // size):
        expand_ref[:, k * size : (k + 1) * size] = chunk(at)
        at += 1
    for k in range(contract_ref.shape[0] // size):
        contract_ref[k * size : (k + 1) * size, :] = chunk(at)
        at += 1
    factors = (own_ref[0].astype(F32) + other_ref[0].astype(F32)) * scale
    channels = left_ref.shape[0]
    for h in range(left_ref.shape[1] // size):
        at = slice(h * size, (h + 1) * size)
        left_ref[:, at] = factors[2 * h * channels : (2 * h + 1) * channels]
        right_ref[:, at] = factors[(2 * h + 1) * channels : (2 * h + 2) * channels]


def unpack(core, own, other, scale, shapes):
    smem = pl.BlockSpec(memory_space=pltpu.SMEM)
    vmem = pl.BlockSpec(memory_space=pltpu.VMEM)
    return pl.pallas_call(
        unpack_kernel,
        in_specs=[smem, vmem, vmem, smem],
        out_specs=[vmem] * len(shapes),
        out_shape=[jax.ShapeDtypeStruct(shape, F32) for shape in shapes],
        compiler_params=pltpu.CompilerParams(vmem_limit_bytes=16 * 1024 * 1024),
        name="unpack",
    )(core, own, other, jnp.full((1,), scale, F32))


def project_kernel(x_ref, gain_ref, first_ref, second_ref, left_ref, right_ref, normed_ref, *halves):
    seqs, residues, features = x_ref.shape
    channels = right_ref.shape[0]
    x = x_ref[...].astype(F32)
    centred = x - jnp.mean(x, axis=-1, keepdims=True)
    variance = jnp.mean(centred * centred, axis=-1, keepdims=True)
    vhat = centred * lax.rsqrt(variance + EPSILON)
    factors = jnp.concatenate([first_ref[...], second_ref[...]], axis=0)
    lanes = halves[0].shape[1]
    rows = (vhat * gain_ref[...][None]).reshape(seqs * residues, features)
    for h, scr in enumerate(halves):
        scr[...] = rows[:, h * lanes : (h + 1) * lanes]
    for r in range(residues):
        normed = jnp.concatenate(
            [scr[pl.ds(r, seqs, stride=residues), :] for scr in halves], axis=1
        ).astype(BF16)
        normed_ref[r] = normed
        both = matmul_nt(factors, normed).astype(BF16)
        left = both[:channels] * (1.0 / seqs)
        for k in range(left_ref.shape[0]):
            left_ref[k, r] = left
        right_ref[:, r, :] = both[channels:]


def project(x, gain, first, second, copies):
    seqs, residues, features = x.shape
    channels = first.shape[0]
    vmem = pl.BlockSpec(memory_space=pltpu.VMEM)
    return pl.pallas_call(
        project_kernel,
        in_specs=[vmem] * 4,
        out_specs=[vmem] * 3,
        out_shape=[
            jax.ShapeDtypeStruct((copies, residues, channels, seqs), BF16),
            jax.ShapeDtypeStruct((channels, residues, seqs), BF16),
            jax.ShapeDtypeStruct((residues, seqs, features), BF16),
        ],
        scratch_shapes=[pltpu.VMEM((seqs * residues, 128), F32)] * (features // 128),
        name="project",
    )(x, gain[None, :], first, second)


def factor_grad_kernel(normed_ref, left_ref, right_ref, weights_ref, out_ref):
    residues, seqs, features = normed_ref.shape
    total = 0.0
    for r in range(residues):
        both = jnp.concatenate([left_ref[r], right_ref[:, r, :]], axis=0)
        total = total + matmul(both, normed_ref[r])
    size = out_ref.shape[2]
    parts = [total[:, k : k + size].astype(BF16) for k in range(0, features, size)]
    rows = jnp.concatenate(parts + [weights_ref[...]], axis=0)
    for k in range(out_ref.shape[0]):
        out_ref[k] = rows


def factor_grad(normed, left, right, weights, copies):
    vmem = pl.BlockSpec(memory_space=pltpu.VMEM)
    lanes = weights.shape[1]
    rows = 2 * right.shape[0] * (normed.shape[2] // lanes) + weights.shape[0]
    return pl.pallas_call(
        factor_grad_kernel,
        in_specs=[vmem] * 4,
        out_specs=vmem,
        out_shape=jax.ShapeDtypeStruct((copies, rows, lanes), BF16),
        compiler_params=pltpu.CompilerParams(vmem_limit_bytes=16 * 1024 * 1024),
        name="factor_grad",
    )(normed, left, right, weights)


def align_grad_kernel(x_ref, gain_ref, first_ref, second_ref, left_ref, right_ref, out_ref, *halves):
    seqs, residues, features = x_ref.shape
    lanes = halves[0].shape[1]
    factors = jnp.concatenate([first_ref[...], second_ref[...]], axis=0)
    for r in range(residues):
        both = jnp.concatenate([left_ref[r], right_ref[:, r, :]], axis=0)
        grad = lax.dot_general(
            both, factors, (((0,), (0,)), ((), ())), preferred_element_type=F32
        )
        for h, scr in enumerate(halves):
            scr[pl.ds(r, seqs, stride=residues), :] = grad[:, h * lanes : (h + 1) * lanes]
    x = x_ref[...].astype(F32)
    centred = x - jnp.mean(x, axis=-1, keepdims=True)
    variance = jnp.mean(centred * centred, axis=-1, keepdims=True)
    inv = lax.rsqrt(variance + EPSILON)
    vhat = centred * inv
    grad = jnp.concatenate([scr[...] for scr in halves], axis=1)
    scaled = grad.reshape(seqs, residues, features) * gain_ref[...][None]
    grad = inv * (
        scaled
        - jnp.mean(scaled, axis=-1, keepdims=True)
        - vhat * jnp.mean(scaled * vhat, axis=-1, keepdims=True)
    )
    out_ref[...] = grad.astype(BF16)


def align_grad(x, gain, first, second, left, right):
    seqs, residues, features = x.shape
    vmem = pl.BlockSpec(memory_space=pltpu.VMEM)
    return pl.pallas_call(
        align_grad_kernel,
        in_specs=[vmem] * 6,
        out_specs=vmem,
        out_shape=jax.ShapeDtypeStruct(x.shape, BF16),
        scratch_shapes=[pltpu.VMEM((seqs * residues, 128), F32)] * (features // 128),
        cost_estimate=pl.CostEstimate(
            flops=300 * x.size, transcendentals=seqs * residues, bytes_accessed=5 * x.size
        ),
        compiler_params=pltpu.CompilerParams(vmem_limit_bytes=16 * 1024 * 1024),
        name="align_grad",
    )(x, gain[None, :], first, second, left, right)


def parity_groups():
    rows = lax.axis_size("row")
    return [list(range(k, rows, 2)) for k in range(2)]


def exchange(x, axis):
    groups = parity_groups() if axis == "row" else None
    return lax.all_to_all(x, axis, 0, 0, tiled=True, axis_index_groups=groups)


def spread(x, axis):
    count = lax.axis_size("row") // 2 if axis == "row" else lax.axis_size(axis)
    return exchange(jnp.broadcast_to(x[None], (count, *x.shape)), axis)


def from_partner(x):
    return lax.ppermute(x, "row", [(k, k ^ 1) for k in range(lax.axis_size("row"))])


def summed(x):
    return jnp.sum(x.astype(F32), axis=0).astype(BF16)


def column_pairs(rows, cols):
    there = [(b, (b % rows) * cols + b // rows) for b in range(rows * cols)]
    return there, [(to, at) for at, to in there]


def on_device(
    alignment_tensor,
    alignment_scaling_vector,
    first_factor_matrix,
    second_factor_matrix,
    final_mapping_matrix,
    final_offset_vector,
    couple_tensor,
    feedforward_scaling_vector,
    feedforward_expand_matrix,
    feedforward_contract_matrix,
    upstream_sensitivity,
):
    aligned_number, shard_extent, features = alignment_tensor.shape
    channels = first_factor_matrix.shape[1]
    row_count, col_count, pair_width = couple_tensor.shape
    rows, cols = lax.axis_size("row"), lax.axis_size("col")
    amino_number = row_count * rows
    gain = alignment_scaling_vector.astype(F32)
    first_t, second_t = first_factor_matrix.T, second_factor_matrix.T
    left_copies, right_local, normed = project(alignment_tensor, gain, first_t, second_t, cols)
    by_e = (
        final_mapping_matrix.reshape(channels, channels, pair_width)
        .transpose(1, 0, 2)
        .reshape(channels * channels, pair_width)
    )
    turned = (by_e, by_e.T, feedforward_expand_matrix.T, feedforward_contract_matrix.T)
    there, back = column_pairs(rows, cols)
    right_moved = lax.ppermute(right_local, BOTH, there)
    left_rows = exchange(left_copies, "col")
    right_moved, left_rows, turned = lax.optimization_barrier((right_moved, left_rows, turned))
    by_e, by_e_t, expand_t, contract_t = turned
    own = spread(right_moved, "row")
    other = from_partner(own)
    core = (lax.axis_index("row") % 2).astype(jnp.int32)[None]
    result, grad, d_left, mine, theirs = pair_stage(
        core,
        left_rows.reshape(row_count * channels, aligned_number),
        own,
        other,
        couple_tensor,
        upstream_sensitivity,
        (by_e, by_e_t, feedforward_expand_matrix, expand_t, feedforward_contract_matrix, contract_t),
        final_offset_vector,
        feedforward_scaling_vector,
        rows * cols,
    )
    lanes = pair_width
    mine = (mine.astype(F32) + from_partner(theirs).astype(F32)).astype(BF16)
    mine = summed(exchange(mine, "row"))
    size = channels * shard_extent
    d_right = mine[:size].reshape(channels, shard_extent, aligned_number)
    with_left = lax.dynamic_update_slice(
        d_left, mine[size:].reshape(cols, -1, lanes), (0, size, 0)
    )
    d_right, with_left = lax.optimization_barrier((d_right, with_left))
    d_right = lax.ppermute(d_right, BOTH, back)
    with_left = summed(exchange(with_left, "col"))
    d_left = with_left[:size].reshape(shard_extent, channels, aligned_number)
    weights = with_left[size:]

    gathered = exchange(factor_grad(normed, d_left, d_right, weights, cols), "col")
    count = gathered.shape[1] - weights.shape[0]
    factors = summed(gathered[:, :count])
    weights = gathered[:, count:].reshape(-1, lanes)
    gathered = spread(jnp.stack([factors, weights], axis=0), "row")
    alignment_sensitivity = align_grad(
        alignment_tensor, gain, first_t, second_t, d_left, d_right
    )
    half = jnp.concatenate([summed(gathered[:, 0])[None], gathered[:, 1]], axis=0)
    half, alignment_sensitivity = lax.optimization_barrier((half, alignment_sensitivity))
    outs = unpack(
        core,
        half,
        from_partner(half),
        1.0 / amino_number,
        (
            final_mapping_matrix.shape,
            feedforward_expand_matrix.shape,
            feedforward_contract_matrix.shape,
            first_factor_matrix.shape[::-1],
            second_factor_matrix.shape[::-1],
        ),
    )
    return (result, grad, alignment_sensitivity, *outs[:3], outs[3].T, outs[4].T)


def solution(mesh):
    return jax.shard_map(
        on_device,
        mesh=mesh,
        in_specs=(
            P(None, ("row", "col"), None),
            P(),
            P(),
            P(),
            P(),
            P(),
            P("row", "col", None),
            P(),
            P(),
            P(),
            P("row", "col", None),
        ),
        out_specs=(
            P("row", "col", None),
            P("row", "col", None),
            P(None, ("row", "col"), None),
            P(),
            P(),
            P(),
            P(),
            P(),
        ),
        check_vma=False,
    )
```

```python
import jax
import jax.numpy as jnp
from jax import lax
from jax.experimental import pallas as pl
from jax.experimental.pallas import tpu as pltpu
from jax.sharding import PartitionSpec as P

EPSILON = 1e-05
ROOT_HALF = 0.7071067811865476
INV_ROOT_TWO_PI = 0.3989422804014327

F32 = jnp.float32
BF16 = jnp.bfloat16
CHUNK = 128
BOTH = ("row", "col")


def matmul(a, b):
    return lax.dot_general(a, b, (((1,), (0,)), ((), ())), preferred_element_type=F32)


def matmul_nt(a, b):
    return lax.dot_general(a, b, (((1,), (1,)), ((), ())), preferred_element_type=F32)


def pair_kernel(
    core_ref,
    left_ref,
    own_ref,
    other_ref,
    pair_ref,
    cot_ref,
    proj_ref,
    proj_t_ref,
    expand_ref,
    expand_t_ref,
    contract_ref,
    contract_t_ref,
    offset_ref,
    gain_ref,
    result_ref,
    grad_ref,
    d_left_ref,
    own_out_ref,
    other_out_ref,
    right_t_scr,
    right_scr,
    outer_scr,
    d_outer_scr,
    acc_right,
    hidden_scr,
    d_hidden_scr,
    acc_left,
    left_t_scr,
    g_proj_ref,
    g_expand_ref,
    g_contract_ref,
):
    step = pl.program_id(0)
    first = core_ref[0] == 0
    block = pair_ref.shape[0]
    seqs = left_ref.shape[1]
    wide = right_t_scr.shape[0]
    width = proj_t_ref.shape[0]
    lanes = pair_ref.shape[1]
    channels = wide // lanes
    rows = block * channels
    blocks = left_ref.shape[0] // rows
    chunk = 2 * lanes

    def left_rows(b):
        return left_ref[pl.ds(pl.multiple_of(b * rows, rows), rows), :]

    def outer_product(b, at):
        outer_scr[:, at] = matmul(left_rows(b), right_scr[:, at]).astype(BF16)

    def pieces(h):
        each = wide // (4 * chunk)
        return [slice((h * each + k) * chunk, (h * each + k + 1) * chunk) for k in range(each)]

    def backward(b, h):
        at = slice(h * wide // 4, (h + 1) * wide // 4)
        part = matmul(d_outer_scr[:, at], right_t_scr[at, :])
        left_t = left_t_scr[...]
        for to in pieces(h):
            acc_right[:, to] += matmul(left_t, d_outer_scr[:, to])
        if h == 0:
            acc_left[...] = part
        elif h < 3:
            acc_left[...] += part
        else:
            total = (acc_left[...] + part) * (1.0 / seqs)
            d_left_ref[b, :rows, :] = total.astype(BF16)

    @pl.when(step == 0)
    def _():
        for e in range(channels):
            at = slice(e * lanes, (e + 1) * lanes)
            own, other = own_ref[:, e], other_ref[:, e]
            both = (jnp.where(first, own, other), jnp.where(first, other, own))
            tile = jnp.stack(both, axis=1).reshape(lanes, seqs)
            right_t_scr[at, :] = tile
            right_scr[:, at] = tile.T
        acc_right[...] = jnp.zeros_like(acc_right)
        d_outer_scr[...] = jnp.zeros_like(d_outer_scr)
        g_proj_ref[...] = jnp.zeros_like(g_proj_ref)
        g_expand_ref[...] = jnp.zeros_like(g_expand_ref)
        g_contract_ref[...] = jnp.zeros_like(g_contract_ref)
        for h in range(4):
            for at in pieces(h):
                outer_product(0, at)

    before = jnp.maximum(step - 1, 0)
    after = jnp.minimum(step + 1, blocks - 1)
    left_t_scr[...] = left_rows(before).T

    gain = jnp.broadcast_to(gain_ref[...], (2 * lanes, width)).T
    offset = jnp.broadcast_to(offset_ref[...], (2 * lanes, width)).T

    def columns(scr, i, some):
        row = slice(i * channels, (i + 1) * channels)
        tiles = [
            scr[row, e * lanes : (e + 1) * lanes] for e in range(some.start, some.stop)
        ]
        return jnp.concatenate(tiles, axis=0)

    def beside(ref, i):
        return jnp.concatenate([ref[i].T, ref[i + 1].T], axis=1)

    scale = 1.0 / width

    def forward(p):
        i = 2 * p
        outer = jnp.concatenate([columns(outer_scr, i + k, slice(0, channels)) for k in range(2)], axis=1)
        update = matmul(proj_t_ref[...], outer) + offset
        middle = (beside(pair_ref, i).astype(F32) + update).astype(BF16).astype(F32)
        average = jnp.sum(middle, axis=0, keepdims=True) * scale
        centred = middle - average
        variance = jnp.sum(centred * centred, axis=0, keepdims=True) * scale
        inv = lax.rsqrt(variance + EPSILON)
        vhat = centred * inv
        normed = (vhat * gain).astype(BF16)
        return dict(p=p, middle=middle, vhat=vhat, inv=inv, normed=normed,
                    cot=beside(cot_ref, i))

    def activate(st, h):
        p = st["p"]
        at = slice(h * CHUNK, (h + 1) * CHUNK)
        pre = matmul(expand_t_ref[at, :], st["normed"])
        half = 0.5 + 0.5 * lax.erf(pre * ROOT_HALF)
        hidden_scr[p, at, :] = (pre * half).astype(BF16)
        slope = half + pre * jnp.exp(-0.5 * pre * pre) * INV_ROOT_TWO_PI
        d_hidden_scr[p, at, :] = (matmul(contract_ref[at, :], st["cot"]) * slope).astype(BF16)

    def through(st):
        p, i = st["p"], 2 * st["p"]
        cot, vhat = st["cot"], st["vhat"]
        q = matmul(expand_ref[...], d_hidden_scr[p]) * gain
        result = (st["middle"] + matmul(contract_t_ref[...], hidden_scr[p])).astype(BF16)
        result_ref[i] = result[:, :lanes].T
        result_ref[i + 1] = result[:, lanes:].T
        q_mean = jnp.sum(q, axis=0, keepdims=True) * scale
        q_hat = jnp.sum(q * vhat, axis=0, keepdims=True) * scale
        grad = (cot.astype(F32) + st["inv"] * (q - q_mean - vhat * q_hat)).astype(BF16)
        grad_ref[i] = grad[:, :lanes].T
        grad_ref[i + 1] = grad[:, lanes:].T
        st["grad"] = grad

    def weigh(st, h):
        p, i = st["p"], 2 * st["p"]
        part = proj_ref.shape[0] // 4
        at = slice(h * part, (h + 1) * part)
        d_outer = matmul(proj_ref[at, :], st["grad"]).astype(BF16)
        for k in range(2):
            row = slice((i + k) * channels, (i + k + 1) * channels)
            for e in range(part // channels):
                to = h * (part // channels) + e
                d_outer_scr[row, to * lanes : (to + 1) * lanes] = d_outer[
                    e * channels : (e + 1) * channels, k * lanes : (k + 1) * lanes
                ]
        some = slice(h * part // channels, (h + 1) * part // channels)
        outer = jnp.concatenate(
            [columns(outer_scr, i, some), columns(outer_scr, i + 1, some)], axis=1
        )
        g_proj_ref[at, :] += matmul_nt(outer, st["grad"])
        at = slice(h * CHUNK, (h + 1) * CHUNK)
        g_contract_ref[at, :] += matmul_nt(hidden_scr[p, at, :], st["cot"])
        g_expand_ref[at, :] += matmul_nt(d_hidden_scr[p, at, :], st["normed"])

    count = block // 2
    ahead, last = forward(0), None
    for p in range(count + 1):
        now = ahead if p < count else None
        if last is not None:
            through(last)
        for h in range(4):
            if p == 0:
                backward(before, h)
            if h == 0 and p + 1 < count:
                ahead = forward(p + 1)
            if now is not None:
                activate(now, h)
            if last is not None:
                pass
                weigh(last, h)
            if p == count:
                for at in pieces(h):
                    outer_product(after, at)
        last = now

    @pl.when(step == pl.num_programs(0) - 1)
    def _():
        left_t_scr[...] = left_rows(step).T
        for h in range(4):
            backward(step, h)
        each = own_ref.shape[2]
        halves = own_ref.shape[0]

        def hand_out(at, even, odd):
            own_out_ref[:, at, :] = jnp.where(first, even, odd).astype(BF16)
            other_out_ref[:, at, :] = jnp.where(first, odd, even).astype(BF16)

        for e in range(channels):
            tile = acc_right[:, e * lanes : (e + 1) * lanes].T.reshape(halves, 2, each, seqs)
            hand_out(slice(e * each, (e + 1) * each), tile[:, 0], tile[:, 1])

        def weight_rows(k):
            full = width
            per = full // channels
            if k < channels // per:
                cs = range(k * per, (k + 1) * per)
                return jnp.concatenate(
                    [g_proj_ref[pl.ds(c, channels, stride=channels), :] for c in cs], axis=0
                )
            k -= channels // per
            at = slice(k * full, (k + 1) * full)
            if k < g_expand_ref.shape[0] // full:
                return g_expand_ref[at, :].T
            at = slice(at.start - g_expand_ref.shape[0], at.stop - g_expand_ref.shape[0])
            return g_contract_ref[at, :]

        base = channels * each
        for m in range(halves):
            even, odd = weight_rows(2 * m), weight_rows(2 * m + 1)
            own_out_ref[m, base:, :] = jnp.where(first, even, odd).astype(BF16)
            other_out_ref[m, base:, :] = jnp.where(first, odd, even).astype(BF16)


def pair_stage(core, left, own, other, pair, cot, weights, offset, gain, devices):
    by_e, by_e_t, expand, expand_t, contract, contract_t = weights
    each = own.shape[2]
    rows, lanes, width = pair.shape
    seqs = left.shape[1]
    channels = own.shape[1]
    wide = channels * lanes
    hidden = expand.shape[1]
    block = 8
    whole = lambda shape: pl.BlockSpec(shape, lambda b: (0,) * len(shape))
    grads = channels * channels + 2 * hidden
    d_left = (rows // block, block * channels + grads // devices, seqs)
    parts = (own.shape[0], channels * each + grads // (2 * own.shape[0]), width)
    tiles = pl.BlockSpec((block, lanes, width), lambda b: (b, 0, 0))
    flat = whole((rows * channels, seqs))
    return pl.pallas_call(
        pair_kernel,
        grid=(rows // block,),
        in_specs=[
            pl.BlockSpec(memory_space=pltpu.SMEM),
            flat,
            whole(own.shape),
            whole(own.shape),
            tiles,
            tiles,
            whole((channels * channels, width)),
            whole((width, channels * channels)),
            whole((width, hidden)),
            whole((hidden, width)),
            whole((hidden, width)),
            whole((width, hidden)),
            whole((1, width)),
            whole((1, width)),
        ],
        out_specs=[
            tiles,
            tiles,
            whole(d_left),
            whole(parts),
            whole(parts),
        ],
        out_shape=[
            jax.ShapeDtypeStruct((rows, lanes, width), BF16),
            jax.ShapeDtypeStruct((rows, lanes, width), BF16),
            jax.ShapeDtypeStruct(d_left, BF16),
            jax.ShapeDtypeStruct(parts, BF16),
            jax.ShapeDtypeStruct(parts, BF16),
        ],
        scratch_shapes=[
            pltpu.VMEM((wide, seqs), BF16),
            pltpu.VMEM((seqs, wide), BF16),
            pltpu.VMEM((block * channels, wide), BF16),
            pltpu.VMEM((block * channels, wide), BF16),
            pltpu.VMEM((seqs, wide), F32),
            pltpu.VMEM((block // 2, hidden, 2 * lanes), BF16),
            pltpu.VMEM((block // 2, hidden, 2 * lanes), BF16),
            pltpu.VMEM((block * channels, seqs), F32),
            pltpu.VMEM((seqs, block * channels), BF16),
            pltpu.VMEM((channels * channels, width), F32),
            pltpu.VMEM((hidden, width), F32),
            pltpu.VMEM((hidden, width), F32),
        ],
        compiler_params=pltpu.CompilerParams(
            dimension_semantics=("arbitrary",), vmem_limit_bytes=56 * 1024 * 1024
        ),
        name="pair_stage",
    )(
        core,
        left,
        own,
        other,
        pair,
        cot,
        *weights,
        offset.astype(F32)[None, :],
        gain.astype(F32)[None, :],
    )


def unpack_kernel(
    core_ref, own_ref, other_ref, scale_ref, proj_ref, expand_ref, contract_ref, left_ref, right_ref
):
    first = core_ref[0] == 0
    size = own_ref.shape[2]
    scale = scale_ref[0]
    halves = own_ref.shape[0] - 1

    def chunk(k):
        own, other = own_ref[1 + k // 2].astype(F32), other_ref[1 + k // 2].astype(F32)
        picked = jnp.where(first, own, other) if k % 2 == 0 else jnp.where(first, other, own)
        return picked * scale

    at = 0
    for k in range(proj_ref.shape[0] // size):
        proj_ref[k * size : (k + 1) * size, :] = chunk(at)
        at += 1
    for k in range(expand_ref.shape[1] // size):
        expand_ref[:, k * size : (k + 1) * size] = chunk(at)
        at += 1
    for k in range(contract_ref.shape[0] // size):
        contract_ref[k * size : (k + 1) * size, :] = chunk(at)
        at += 1
    factors = (own_ref[0].astype(F32) + other_ref[0].astype(F32)) * scale
    channels = left_ref.shape[0]
    for h in range(left_ref.shape[1] // size):
        at = slice(h * size, (h + 1) * size)
        left_ref[:, at] = factors[2 * h * channels : (2 * h + 1) * channels]
        right_ref[:, at] = factors[(2 * h + 1) * channels : (2 * h + 2) * channels]


def unpack(core, own, other, scale, shapes):
    smem = pl.BlockSpec(memory_space=pltpu.SMEM)
    vmem = pl.BlockSpec(memory_space=pltpu.VMEM)
    return pl.pallas_call(
        unpack_kernel,
        in_specs=[smem, vmem, vmem, smem],
        out_specs=[vmem] * len(shapes),
        out_shape=[jax.ShapeDtypeStruct(shape, F32) for shape in shapes],
        compiler_params=pltpu.CompilerParams(vmem_limit_bytes=16 * 1024 * 1024),
        name="unpack",
    )(core, own, other, jnp.full((1,), scale, F32))


def project_kernel(x_ref, gain_ref, first_ref, second_ref, left_ref, right_ref, normed_ref, *halves):
    seqs, residues, features = x_ref.shape
    channels = right_ref.shape[0]
    x = x_ref[...].astype(F32)
    centred = x - jnp.mean(x, axis=-1, keepdims=True)
    variance = jnp.mean(centred * centred, axis=-1, keepdims=True)
    vhat = centred * lax.rsqrt(variance + EPSILON)
    factors = jnp.concatenate([first_ref[...], second_ref[...]], axis=0)
    lanes = halves[0].shape[1]
    rows = (vhat * gain_ref[...][None]).reshape(seqs * residues, features)
    for h, scr in enumerate(halves):
        scr[...] = rows[:, h * lanes : (h + 1) * lanes]
    for r in range(residues):
        normed = jnp.concatenate(
            [scr[pl.ds(r, seqs, stride=residues), :] for scr in halves], axis=1
        ).astype(BF16)
        normed_ref[r] = normed
        both = matmul_nt(factors, normed).astype(BF16)
        left = both[:channels] * (1.0 / seqs)
        for k in range(left_ref.shape[0]):
            left_ref[k, r] = left
        right_ref[:, r, :] = both[channels:]


def project(x, gain, first, second, copies):
    seqs, residues, features = x.shape
    channels = first.shape[0]
    vmem = pl.BlockSpec(memory_space=pltpu.VMEM)
    return pl.pallas_call(
        project_kernel,
        in_specs=[vmem] * 4,
        out_specs=[vmem] * 3,
        out_shape=[
            jax.ShapeDtypeStruct((copies, residues, channels, seqs), BF16),
            jax.ShapeDtypeStruct((channels, residues, seqs), BF16),
            jax.ShapeDtypeStruct((residues, seqs, features), BF16),
        ],
        scratch_shapes=[pltpu.VMEM((seqs * residues, 128), F32)] * (features // 128),
        name="project",
    )(x, gain[None, :], first, second)


def factor_grad_kernel(normed_ref, left_ref, right_ref, weights_ref, out_ref):
    residues, seqs, features = normed_ref.shape
    total = 0.0
    for r in range(residues):
        both = jnp.concatenate([left_ref[r], right_ref[:, r, :]], axis=0)
        total = total + matmul(both, normed_ref[r])
    size = out_ref.shape[2]
    parts = [total[:, k : k + size].astype(BF16) for k in range(0, features, size)]
    rows = jnp.concatenate(parts + [weights_ref[...]], axis=0)
    for k in range(out_ref.shape[0]):
        out_ref[k] = rows


def factor_grad(normed, left, right, weights, copies):
    vmem = pl.BlockSpec(memory_space=pltpu.VMEM)
    lanes = weights.shape[1]
    rows = 2 * right.shape[0] * (normed.shape[2] // lanes) + weights.shape[0]
    return pl.pallas_call(
        factor_grad_kernel,
        in_specs=[vmem] * 4,
        out_specs=vmem,
        out_shape=jax.ShapeDtypeStruct((copies, rows, lanes), BF16),
        compiler_params=pltpu.CompilerParams(vmem_limit_bytes=16 * 1024 * 1024),
        name="factor_grad",
    )(normed, left, right, weights)


def align_grad_kernel(x_ref, gain_ref, first_ref, second_ref, left_ref, right_ref, out_ref, *halves):
    seqs, residues, features = x_ref.shape
    lanes = halves[0].shape[1]
    factors = jnp.concatenate([first_ref[...], second_ref[...]], axis=0)
    for r in range(residues):
        both = jnp.concatenate([left_ref[r], right_ref[:, r, :]], axis=0)
        grad = lax.dot_general(
            both, factors, (((0,), (0,)), ((), ())), preferred_element_type=F32
        )
        for h, scr in enumerate(halves):
            scr[pl.ds(r, seqs, stride=residues), :] = grad[:, h * lanes : (h + 1) * lanes]
    x = x_ref[...].astype(F32)
    centred = x - jnp.mean(x, axis=-1, keepdims=True)
    variance = jnp.mean(centred * centred, axis=-1, keepdims=True)
    inv = lax.rsqrt(variance + EPSILON)
    vhat = centred * inv
    grad = jnp.concatenate([scr[...] for scr in halves], axis=1)
    scaled = grad.reshape(seqs, residues, features) * gain_ref[...][None]
    grad = inv * (
        scaled
        - jnp.mean(scaled, axis=-1, keepdims=True)
        - vhat * jnp.mean(scaled * vhat, axis=-1, keepdims=True)
    )
    out_ref[...] = grad.astype(BF16)


def align_grad(x, gain, first, second, left, right):
    seqs, residues, features = x.shape
    vmem = pl.BlockSpec(memory_space=pltpu.VMEM)
    return pl.pallas_call(
        align_grad_kernel,
        in_specs=[vmem] * 6,
        out_specs=vmem,
        out_shape=jax.ShapeDtypeStruct(x.shape, BF16),
        scratch_shapes=[pltpu.VMEM((seqs * residues, 128), F32)] * (features // 128),
        cost_estimate=pl.CostEstimate(
            flops=300 * x.size, transcendentals=seqs * residues, bytes_accessed=5 * x.size
        ),
        compiler_params=pltpu.CompilerParams(vmem_limit_bytes=16 * 1024 * 1024),
        name="align_grad",
    )(x, gain[None, :], first, second, left, right)


def parity_groups():
    rows = lax.axis_size("row")
    return [list(range(k, rows, 2)) for k in range(2)]


def exchange(x, axis):
    groups = parity_groups() if axis == "row" else None
    return lax.all_to_all(x, axis, 0, 0, tiled=True, axis_index_groups=groups)


def spread(x, axis):
    count = lax.axis_size("row") // 2 if axis == "row" else lax.axis_size(axis)
    return exchange(jnp.broadcast_to(x[None], (count, *x.shape)), axis)


def from_partner(x):
    return lax.ppermute(x, "row", [(k, k ^ 1) for k in range(lax.axis_size("row"))])


def summed(x):
    return jnp.sum(x.astype(F32), axis=0).astype(BF16)


def column_pairs(rows, cols):
    there = [(b, (b % rows) * cols + b // rows) for b in range(rows * cols)]
    return there, [(to, at) for at, to in there]


def on_device(
    alignment_tensor,
    alignment_scaling_vector,
    first_factor_matrix,
    second_factor_matrix,
    final_mapping_matrix,
    final_offset_vector,
    couple_tensor,
    feedforward_scaling_vector,
    feedforward_expand_matrix,
    feedforward_contract_matrix,
    upstream_sensitivity,
):
    aligned_number, shard_extent, features = alignment_tensor.shape
    channels = first_factor_matrix.shape[1]
    row_count, col_count, pair_width = couple_tensor.shape
    rows, cols = lax.axis_size("row"), lax.axis_size("col")
    amino_number = row_count * rows
    gain = alignment_scaling_vector.astype(F32)
    first_t, second_t = first_factor_matrix.T, second_factor_matrix.T
    left_copies, right_local, normed = project(alignment_tensor, gain, first_t, second_t, cols)
    by_e = (
        final_mapping_matrix.reshape(channels, channels, pair_width)
        .transpose(1, 0, 2)
        .reshape(channels * channels, pair_width)
    )
    turned = (by_e, by_e.T, feedforward_expand_matrix.T, feedforward_contract_matrix.T)
    there, back = column_pairs(rows, cols)
    right_moved = lax.ppermute(right_local, BOTH, there)
    left_rows = exchange(left_copies, "col")
    right_moved, left_rows, turned = lax.optimization_barrier((right_moved, left_rows, turned))
    by_e, by_e_t, expand_t, contract_t = turned
    own = spread(right_moved, "row")
    other = from_partner(own)
    core = (lax.axis_index("row") % 2).astype(jnp.int32)[None]
    result, grad, d_left, mine, theirs = pair_stage(
        core,
        left_rows.reshape(row_count * channels, aligned_number),
        own,
        other,
        couple_tensor,
        upstream_sensitivity,
        (by_e, by_e_t, feedforward_expand_matrix, expand_t, feedforward_contract_matrix, contract_t),
        final_offset_vector,
        feedforward_scaling_vector,
        rows * cols,
    )
    lanes = pair_width
    mine = (mine.astype(F32) + from_partner(theirs).astype(F32)).astype(BF16)
    mine = summed(exchange(mine, "row"))
    size = channels * shard_extent
    d_right = mine[:size].reshape(channels, shard_extent, aligned_number)
    with_left = lax.dynamic_update_slice(
        d_left, mine[size:].reshape(cols, -1, lanes), (0, size, 0)
    )
    d_right, with_left = lax.optimization_barrier((d_right, with_left))
    d_right = lax.ppermute(d_right, BOTH, back)
    with_left = summed(exchange(with_left, "col"))
    d_left = with_left[:size].reshape(shard_extent, channels, aligned_number)
    weights = with_left[size:]

    gathered = exchange(factor_grad(normed, d_left, d_right, weights, cols), "col")
    count = gathered.shape[1] - weights.shape[0]
    factors = summed(gathered[:, :count])
    weights = gathered[:, count:].reshape(-1, lanes)
    gathered = spread(jnp.stack([factors, weights], axis=0), "row")
    alignment_sensitivity = align_grad(
        alignment_tensor, gain, first_t, second_t, d_left, d_right
    )
    half = jnp.concatenate([summed(gathered[:, 0])[None], gathered[:, 1]], axis=0)
    half, alignment_sensitivity = lax.optimization_barrier((half, alignment_sensitivity))
    outs = unpack(
        core,
        half,
        from_partner(half),
        1.0 / amino_number,
        (
            final_mapping_matrix.shape,
            feedforward_expand_matrix.shape,
            feedforward_contract_matrix.shape,
            first_factor_matrix.shape[::-1],
            second_factor_matrix.shape[::-1],
        ),
    )
    return (result, grad, alignment_sensitivity, *outs[:3], outs[3].T, outs[4].T)


def solution(mesh):
    return jax.shard_map(
        on_device,
        mesh=mesh,
        in_specs=(
            P(None, ("row", "col"), None),
            P(),
            P(),
            P(),
            P(),
            P(),
            P("row", "col", None),
            P(),
            P(),
            P(),
            P("row", "col", None),
        ),
        out_specs=(
            P("row", "col", None),
            P("row", "col", None),
            P(None, ("row", "col"), None),
            P(),
            P(),
            P(),
            P(),
            P(),
        ),
        check_vma=False,
    )
```

```python
import jax
import jax.numpy as jnp
from jax import lax
from jax.experimental import pallas as pl
from jax.experimental.pallas import tpu as pltpu
from jax.sharding import PartitionSpec as P

EPSILON = 1e-05
ROOT_HALF = 0.7071067811865476
INV_ROOT_TWO_PI = 0.3989422804014327

F32 = jnp.float32
BF16 = jnp.bfloat16
CHUNK = 128
BOTH = ("row", "col")


def matmul(a, b):
    return lax.dot_general(a, b, (((1,), (0,)), ((), ())), preferred_element_type=F32)


def matmul_nt(a, b):
    return lax.dot_general(a, b, (((1,), (1,)), ((), ())), preferred_element_type=F32)


def pair_kernel(
    core_ref,
    left_ref,
    own_ref,
    other_ref,
    pair_ref,
    cot_ref,
    proj_ref,
    proj_t_ref,
    expand_ref,
    expand_t_ref,
    contract_ref,
    contract_t_ref,
    offset_ref,
    gain_ref,
    result_ref,
    grad_ref,
    d_left_ref,
    own_out_ref,
    other_out_ref,
    right_t_scr,
    right_scr,
    outer_scr,
    d_outer_scr,
    acc_right,
    hidden_scr,
    d_hidden_scr,
    acc_left,
    left_t_scr,
    g_proj_ref,
    g_expand_ref,
    g_contract_ref,
):
    step = pl.program_id(0)
    first = core_ref[0] == 0
    block = pair_ref.shape[0]
    seqs = left_ref.shape[1]
    wide = right_t_scr.shape[0]
    width = proj_t_ref.shape[0]
    lanes = pair_ref.shape[1]
    channels = wide // lanes
    rows = block * channels
    blocks = left_ref.shape[0] // rows
    chunk = 2 * lanes

    def left_rows(b):
        return left_ref[pl.ds(pl.multiple_of(b * rows, rows), rows), :]

    def outer_product(b, at):
        outer_scr[:, at] = matmul(left_rows(b), right_scr[:, at]).astype(BF16)

    def pieces(h):
        each = wide // (4 * chunk)
        return [slice((h * each + k) * chunk, (h * each + k + 1) * chunk) for k in range(each)]

    def backward(b, h):
        at = slice(h * wide // 4, (h + 1) * wide // 4)
        part = matmul(d_outer_scr[:, at], right_t_scr[at, :])
        left_t = left_t_scr[...]
        for to in pieces(h):
            acc_right[:, to] += matmul(left_t, d_outer_scr[:, to])
        if h == 0:
            acc_left[...] = part
        elif h < 3:
            acc_left[...] += part
        else:
            total = (acc_left[...] + part) * (1.0 / seqs)
            d_left_ref[b, :rows, :] = total.astype(BF16)

    @pl.when(step == 0)
    def _():
        for e in range(channels):
            at = slice(e * lanes, (e + 1) * lanes)
            own, other = own_ref[:, e], other_ref[:, e]
            both = (jnp.where(first, own, other), jnp.where(first, other, own))
            tile = jnp.stack(both, axis=1).reshape(lanes, seqs)
            right_t_scr[at, :] = tile
            right_scr[:, at] = tile.T
        acc_right[...] = jnp.zeros_like(acc_right)
        d_outer_scr[...] = jnp.zeros_like(d_outer_scr)
        g_proj_ref[...] = jnp.zeros_like(g_proj_ref)
        g_expand_ref[...] = jnp.zeros_like(g_expand_ref)
        g_contract_ref[...] = jnp.zeros_like(g_contract_ref)
        for h in range(4):
            for at in pieces(h):
                outer_product(0, at)

    before = jnp.maximum(step - 1, 0)
    after = jnp.minimum(step + 1, blocks - 1)
    left_t_scr[...] = left_rows(before).T

    gain = jnp.broadcast_to(gain_ref[...], (2 * lanes, width)).T
    offset = jnp.broadcast_to(offset_ref[...], (2 * lanes, width)).T

    def columns(scr, i, some):
        row = slice(i * channels, (i + 1) * channels)
        tiles = [
            scr[row, e * lanes : (e + 1) * lanes] for e in range(some.start, some.stop)
        ]
        return jnp.concatenate(tiles, axis=0)

    def beside(ref, i):
        return jnp.concatenate([ref[i].T, ref[i + 1].T], axis=1)

    scale = 1.0 / width

    def forward(p):
        i = 2 * p
        outer = jnp.concatenate([columns(outer_scr, i + k, slice(0, channels)) for k in range(2)], axis=1)
        update = matmul(proj_t_ref[...], outer) + offset
        middle = (beside(pair_ref, i).astype(F32) + update).astype(BF16).astype(F32)
        average = jnp.sum(middle, axis=0, keepdims=True) * scale
        centred = middle - average
        variance = jnp.sum(centred * centred, axis=0, keepdims=True) * scale
        inv = lax.rsqrt(variance + EPSILON)
        vhat = centred * inv
        normed = (vhat * gain).astype(BF16)
        return dict(p=p, middle=middle, vhat=vhat, inv=inv, normed=normed,
                    cot=beside(cot_ref, i))

    def activate(st, h):
        p = st["p"]
        at = slice(h * CHUNK, (h + 1) * CHUNK)
        pre = matmul(expand_t_ref[at, :], st["normed"])
        half = 0.5 + 0.5 * lax.erf(pre * ROOT_HALF)
        hidden_scr[p, at, :] = (pre * half).astype(BF16)
        slope = half + pre * jnp.exp(-0.5 * pre * pre) * INV_ROOT_TWO_PI
        d_hidden_scr[p, at, :] = (matmul(contract_ref[at, :], st["cot"]) * slope).astype(BF16)

    def through(st):
        p, i = st["p"], 2 * st["p"]
        cot, vhat = st["cot"], st["vhat"]
        q = matmul(expand_ref[...], d_hidden_scr[p]) * gain
        result = (st["middle"] + matmul(contract_t_ref[...], hidden_scr[p])).astype(BF16)
        result_ref[i] = result[:, :lanes].T
        result_ref[i + 1] = result[:, lanes:].T
        q_mean = jnp.sum(q, axis=0, keepdims=True) * scale
        q_hat = jnp.sum(q * vhat, axis=0, keepdims=True) * scale
        grad = (cot.astype(F32) + st["inv"] * (q - q_mean - vhat * q_hat)).astype(BF16)
        grad_ref[i] = grad[:, :lanes].T
        grad_ref[i + 1] = grad[:, lanes:].T
        st["grad"] = grad

    def weigh(st, h):
        p, i = st["p"], 2 * st["p"]
        part = proj_ref.shape[0] // 4
        at = slice(h * part, (h + 1) * part)
        d_outer = matmul(proj_ref[at, :], st["grad"]).astype(BF16)
        for k in range(2):
            row = slice((i + k) * channels, (i + k + 1) * channels)
            for e in range(part // channels):
                to = h * (part // channels) + e
                d_outer_scr[row, to * lanes : (to + 1) * lanes] = d_outer[
                    e * channels : (e + 1) * channels, k * lanes : (k + 1) * lanes
                ]
        some = slice(h * part // channels, (h + 1) * part // channels)
        outer = jnp.concatenate(
            [columns(outer_scr, i, some), columns(outer_scr, i + 1, some)], axis=1
        )
        g_proj_ref[at, :] += matmul_nt(outer, st["grad"])
        at = slice(h * CHUNK, (h + 1) * CHUNK)
        g_contract_ref[at, :] += matmul_nt(hidden_scr[p, at, :], st["cot"])
        g_expand_ref[at, :] += matmul_nt(d_hidden_scr[p, at, :], st["normed"])

    count = block // 2
    ahead, last = forward(0), None
    for p in range(count + 1):
        now = ahead if p < count else None
        if last is not None:
            through(last)
        for h in range(4):
            if h == 0 and p + 1 < count:
                ahead = forward(p + 1)
            if p == 0:
                backward(before, h)
            if now is not None:
                activate(now, h)
            if last is not None:
                pass
                weigh(last, h)
            if p == count:
                for at in pieces(h):
                    outer_product(after, at)
        last = now

    @pl.when(step == pl.num_programs(0) - 1)
    def _():
        left_t_scr[...] = left_rows(step).T
        for h in range(4):
            backward(step, h)
        each = own_ref.shape[2]
        halves = own_ref.shape[0]

        def hand_out(at, even, odd):
            own_out_ref[:, at, :] = jnp.where(first, even, odd).astype(BF16)
            other_out_ref[:, at, :] = jnp.where(first, odd, even).astype(BF16)

        for e in range(channels):
            tile = acc_right[:, e * lanes : (e + 1) * lanes].T.reshape(halves, 2, each, seqs)
            hand_out(slice(e * each, (e + 1) * each), tile[:, 0], tile[:, 1])

        def weight_rows(k):
            full = width
            per = full // channels
            if k < channels // per:
                cs = range(k * per, (k + 1) * per)
                return jnp.concatenate(
                    [g_proj_ref[pl.ds(c, channels, stride=channels), :] for c in cs], axis=0
                )
            k -= channels // per
            at = slice(k * full, (k + 1) * full)
            if k < g_expand_ref.shape[0] // full:
                return g_expand_ref[at, :].T
            at = slice(at.start - g_expand_ref.shape[0], at.stop - g_expand_ref.shape[0])
            return g_contract_ref[at, :]

        base = channels * each
        for m in range(halves):
            even, odd = weight_rows(2 * m), weight_rows(2 * m + 1)
            own_out_ref[m, base:, :] = jnp.where(first, even, odd).astype(BF16)
            other_out_ref[m, base:, :] = jnp.where(first, odd, even).astype(BF16)


def pair_stage(core, left, own, other, pair, cot, weights, offset, gain, devices):
    by_e, by_e_t, expand, expand_t, contract, contract_t = weights
    each = own.shape[2]
    rows, lanes, width = pair.shape
    seqs = left.shape[1]
    channels = own.shape[1]
    wide = channels * lanes
    hidden = expand.shape[1]
    block = 8
    whole = lambda shape: pl.BlockSpec(shape, lambda b: (0,) * len(shape))
    grads = channels * channels + 2 * hidden
    d_left = (rows // block, block * channels + grads // devices, seqs)
    parts = (own.shape[0], channels * each + grads // (2 * own.shape[0]), width)
    tiles = pl.BlockSpec((block, lanes, width), lambda b: (b, 0, 0))
    flat = whole((rows * channels, seqs))
    return pl.pallas_call(
        pair_kernel,
        grid=(rows // block,),
        in_specs=[
            pl.BlockSpec(memory_space=pltpu.SMEM),
            flat,
            whole(own.shape),
            whole(own.shape),
            tiles,
            tiles,
            whole((channels * channels, width)),
            whole((width, channels * channels)),
            whole((width, hidden)),
            whole((hidden, width)),
            whole((hidden, width)),
            whole((width, hidden)),
            whole((1, width)),
            whole((1, width)),
        ],
        out_specs=[
            tiles,
            tiles,
            whole(d_left),
            whole(parts),
            whole(parts),
        ],
        out_shape=[
            jax.ShapeDtypeStruct((rows, lanes, width), BF16),
            jax.ShapeDtypeStruct((rows, lanes, width), BF16),
            jax.ShapeDtypeStruct(d_left, BF16),
            jax.ShapeDtypeStruct(parts, BF16),
            jax.ShapeDtypeStruct(parts, BF16),
        ],
        scratch_shapes=[
            pltpu.VMEM((wide, seqs), BF16),
            pltpu.VMEM((seqs, wide), BF16),
            pltpu.VMEM((block * channels, wide), BF16),
            pltpu.VMEM((block * channels, wide), BF16),
            pltpu.VMEM((seqs, wide), F32),
            pltpu.VMEM((block // 2, hidden, 2 * lanes), BF16),
            pltpu.VMEM((block // 2, hidden, 2 * lanes), BF16),
            pltpu.VMEM((block * channels, seqs), F32),
            pltpu.VMEM((seqs, block * channels), BF16),
            pltpu.VMEM((channels * channels, width), F32),
            pltpu.VMEM((hidden, width), F32),
            pltpu.VMEM((hidden, width), F32),
        ],
        compiler_params=pltpu.CompilerParams(
            dimension_semantics=("arbitrary",), vmem_limit_bytes=56 * 1024 * 1024
        ),
        name="pair_stage",
    )(
        core,
        left,
        own,
        other,
        pair,
        cot,
        *weights,
        offset.astype(F32)[None, :],
        gain.astype(F32)[None, :],
    )


def unpack_kernel(
    core_ref, own_ref, other_ref, scale_ref, proj_ref, expand_ref, contract_ref, left_ref, right_ref
):
    first = core_ref[0] == 0
    size = own_ref.shape[2]
    scale = scale_ref[0]
    halves = own_ref.shape[0] - 1

    def chunk(k):
        own, other = own_ref[1 + k // 2].astype(F32), other_ref[1 + k // 2].astype(F32)
        picked = jnp.where(first, own, other) if k % 2 == 0 else jnp.where(first, other, own)
        return picked * scale

    at = 0
    for k in range(proj_ref.shape[0] // size):
        proj_ref[k * size : (k + 1) * size, :] = chunk(at)
        at += 1
    for k in range(expand_ref.shape[1] // size):
        expand_ref[:, k * size : (k + 1) * size] = chunk(at)
        at += 1
    for k in range(contract_ref.shape[0] // size):
        contract_ref[k * size : (k + 1) * size, :] = chunk(at)
        at += 1
    factors = (own_ref[0].astype(F32) + other_ref[0].astype(F32)) * scale
    channels = left_ref.shape[0]
    for h in range(left_ref.shape[1] // size):
        at = slice(h * size, (h + 1) * size)
        left_ref[:, at] = factors[2 * h * channels : (2 * h + 1) * channels]
        right_ref[:, at] = factors[(2 * h + 1) * channels : (2 * h + 2) * channels]


def unpack(core, own, other, scale, shapes):
    smem = pl.BlockSpec(memory_space=pltpu.SMEM)
    vmem = pl.BlockSpec(memory_space=pltpu.VMEM)
    return pl.pallas_call(
        unpack_kernel,
        in_specs=[smem, vmem, vmem, smem],
        out_specs=[vmem] * len(shapes),
        out_shape=[jax.ShapeDtypeStruct(shape, F32) for shape in shapes],
        compiler_params=pltpu.CompilerParams(vmem_limit_bytes=16 * 1024 * 1024),
        name="unpack",
    )(core, own, other, jnp.full((1,), scale, F32))


def project_kernel(x_ref, gain_ref, first_ref, second_ref, left_ref, right_ref, normed_ref, *halves):
    seqs, residues, features = x_ref.shape
    channels = right_ref.shape[0]
    x = x_ref[...].astype(F32)
    centred = x - jnp.mean(x, axis=-1, keepdims=True)
    variance = jnp.mean(centred * centred, axis=-1, keepdims=True)
    vhat = centred * lax.rsqrt(variance + EPSILON)
    factors = jnp.concatenate([first_ref[...], second_ref[...]], axis=0)
    lanes = halves[0].shape[1]
    rows = (vhat * gain_ref[...][None]).reshape(seqs * residues, features)
    for h, scr in enumerate(halves):
        scr[...] = rows[:, h * lanes : (h + 1) * lanes]
    for r in range(residues):
        normed = jnp.concatenate(
            [scr[pl.ds(r, seqs, stride=residues), :] for scr in halves], axis=1
        ).astype(BF16)
        normed_ref[r] = normed
        both = matmul_nt(factors, normed).astype(BF16)
        left = both[:channels] * (1.0 / seqs)
        for k in range(left_ref.shape[0]):
            left_ref[k, r] = left
        right_ref[:, r, :] = both[channels:]


def project(x, gain, first, second, copies):
    seqs, residues, features = x.shape
    channels = first.shape[0]
    vmem = pl.BlockSpec(memory_space=pltpu.VMEM)
    return pl.pallas_call(
        project_kernel,
        in_specs=[vmem] * 4,
        out_specs=[vmem] * 3,
        out_shape=[
            jax.ShapeDtypeStruct((copies, residues, channels, seqs), BF16),
            jax.ShapeDtypeStruct((channels, residues, seqs), BF16),
            jax.ShapeDtypeStruct((residues, seqs, features), BF16),
        ],
        scratch_shapes=[pltpu.VMEM((seqs * residues, 128), F32)] * (features // 128),
        name="project",
    )(x, gain[None, :], first, second)


def factor_grad_kernel(normed_ref, left_ref, right_ref, weights_ref, out_ref):
    residues, seqs, features = normed_ref.shape
    total = 0.0
    for r in range(residues):
        both = jnp.concatenate([left_ref[r], right_ref[:, r, :]], axis=0)
        total = total + matmul(both, normed_ref[r])
    size = out_ref.shape[2]
    parts = [total[:, k : k + size].astype(BF16) for k in range(0, features, size)]
    rows = jnp.concatenate(parts + [weights_ref[...]], axis=0)
    for k in range(out_ref.shape[0]):
        out_ref[k] = rows


def factor_grad(normed, left, right, weights, copies):
    vmem = pl.BlockSpec(memory_space=pltpu.VMEM)
    lanes = weights.shape[1]
    rows = 2 * right.shape[0] * (normed.shape[2] // lanes) + weights.shape[0]
    return pl.pallas_call(
        factor_grad_kernel,
        in_specs=[vmem] * 4,
        out_specs=vmem,
        out_shape=jax.ShapeDtypeStruct((copies, rows, lanes), BF16),
        compiler_params=pltpu.CompilerParams(vmem_limit_bytes=16 * 1024 * 1024),
        name="factor_grad",
    )(normed, left, right, weights)


def regroup_kernel(parts_ref, out_ref):
    count = out_ref.shape[2]
    factors = jnp.sum(parts_ref[:, :count, :].astype(F32), axis=0).astype(BF16)
    weights = parts_ref[:, count:, :].reshape(out_ref.shape[2:])
    for k in range(out_ref.shape[0]):
        out_ref[k, 0] = factors
        out_ref[k, 1] = weights


def regroup(parts, count, copies):
    vmem = pl.BlockSpec(memory_space=pltpu.VMEM)
    return pl.pallas_call(
        regroup_kernel,
        in_specs=[vmem],
        out_specs=vmem,
        out_shape=jax.ShapeDtypeStruct((copies, 2, count, parts.shape[2]), BF16),
        compiler_params=pltpu.CompilerParams(vmem_limit_bytes=16 * 1024 * 1024),
        name="regroup",
    )(parts)


def align_grad_kernel(x_ref, gain_ref, first_ref, second_ref, left_ref, right_ref, out_ref, *halves):
    seqs, residues, features = x_ref.shape
    lanes = halves[0].shape[1]
    factors = jnp.concatenate([first_ref[...], second_ref[...]], axis=0)
    for r in range(residues):
        both = jnp.concatenate([left_ref[r], right_ref[:, r, :]], axis=0)
        grad = lax.dot_general(
            both, factors, (((0,), (0,)), ((), ())), preferred_element_type=F32
        )
        for h, scr in enumerate(halves):
            scr[pl.ds(r, seqs, stride=residues), :] = grad[:, h * lanes : (h + 1) * lanes]
    x = x_ref[...].astype(F32)
    centred = x - jnp.mean(x, axis=-1, keepdims=True)
    variance = jnp.mean(centred * centred, axis=-1, keepdims=True)
    inv = lax.rsqrt(variance + EPSILON)
    vhat = centred * inv
    grad = jnp.concatenate([scr[...] for scr in halves], axis=1)
    scaled = grad.reshape(seqs, residues, features) * gain_ref[...][None]
    grad = inv * (
        scaled
        - jnp.mean(scaled, axis=-1, keepdims=True)
        - vhat * jnp.mean(scaled * vhat, axis=-1, keepdims=True)
    )
    out_ref[...] = grad.astype(BF16)


def align_grad(x, gain, first, second, left, right):
    seqs, residues, features = x.shape
    vmem = pl.BlockSpec(memory_space=pltpu.VMEM)
    return pl.pallas_call(
        align_grad_kernel,
        in_specs=[vmem] * 6,
        out_specs=vmem,
        out_shape=jax.ShapeDtypeStruct(x.shape, BF16),
        scratch_shapes=[pltpu.VMEM((seqs * residues, 128), F32)] * (features // 128),
        cost_estimate=pl.CostEstimate(
            flops=300 * x.size, transcendentals=seqs * residues, bytes_accessed=5 * x.size
        ),
        compiler_params=pltpu.CompilerParams(vmem_limit_bytes=16 * 1024 * 1024),
        name="align_grad",
    )(x, gain[None, :], first, second, left, right)


def parity_groups():
    rows = lax.axis_size("row")
    return [list(range(k, rows, 2)) for k in range(2)]


def exchange(x, axis):
    groups = parity_groups() if axis == "row" else None
    return lax.all_to_all(x, axis, 0, 0, tiled=True, axis_index_groups=groups)


def spread(x, axis):
    count = lax.axis_size("row") // 2 if axis == "row" else lax.axis_size(axis)
    return exchange(jnp.broadcast_to(x[None], (count, *x.shape)), axis)


def from_partner(x):
    return lax.ppermute(x, "row", [(k, k ^ 1) for k in range(lax.axis_size("row"))])


def summed(x):
    return jnp.sum(x.astype(F32), axis=0).astype(BF16)


def column_pairs(rows, cols):
    there = [(b, (b % rows) * cols + b // rows) for b in range(rows * cols)]
    return there, [(to, at) for at, to in there]


def on_device(
    alignment_tensor,
    alignment_scaling_vector,
    first_factor_matrix,
    second_factor_matrix,
    final_mapping_matrix,
    final_offset_vector,
    couple_tensor,
    feedforward_scaling_vector,
    feedforward_expand_matrix,
    feedforward_contract_matrix,
    upstream_sensitivity,
):
    aligned_number, shard_extent, features = alignment_tensor.shape
    channels = first_factor_matrix.shape[1]
    row_count, col_count, pair_width = couple_tensor.shape
    rows, cols = lax.axis_size("row"), lax.axis_size("col")
    amino_number = row_count * rows
    gain = alignment_scaling_vector.astype(F32)
    first_t, second_t = first_factor_matrix.T, second_factor_matrix.T
    left_copies, right_local, normed = project(alignment_tensor, gain, first_t, second_t, cols)
    by_e = (
        final_mapping_matrix.reshape(channels, channels, pair_width)
        .transpose(1, 0, 2)
        .reshape(channels * channels, pair_width)
    )
    turned = (by_e, by_e.T, feedforward_expand_matrix.T, feedforward_contract_matrix.T)
    there, back = column_pairs(rows, cols)
    right_moved = lax.ppermute(right_local, BOTH, there)
    left_rows = exchange(left_copies, "col")
    right_moved, left_rows, turned = lax.optimization_barrier((right_moved, left_rows, turned))
    by_e, by_e_t, expand_t, contract_t = turned
    own = spread(right_moved, "row")
    other = from_partner(own)
    core = (lax.axis_index("row") % 2).astype(jnp.int32)[None]
    result, grad, d_left, mine, theirs = pair_stage(
        core,
        left_rows.reshape(row_count * channels, aligned_number),
        own,
        other,
        couple_tensor,
        upstream_sensitivity,
        (by_e, by_e_t, feedforward_expand_matrix, expand_t, feedforward_contract_matrix, contract_t),
        final_offset_vector,
        feedforward_scaling_vector,
        rows * cols,
    )
    lanes = pair_width
    mine = (mine.astype(F32) + from_partner(theirs).astype(F32)).astype(BF16)
    mine = summed(exchange(mine, "row"))
    size = channels * shard_extent
    d_right = mine[:size].reshape(channels, shard_extent, aligned_number)
    with_left = lax.dynamic_update_slice(
        d_left, mine[size:].reshape(cols, -1, lanes), (0, size, 0)
    )
    d_right, with_left = lax.optimization_barrier((d_right, with_left))
    d_right = lax.ppermute(d_right, BOTH, back)
    with_left = summed(exchange(with_left, "col"))
    d_left = with_left[:size].reshape(shard_extent, channels, aligned_number)
    weights = with_left[size:]

    gathered = exchange(factor_grad(normed, d_left, d_right, weights, cols), "col")
    count = gathered.shape[1] - weights.shape[0]
    gathered = exchange(regroup(gathered, count, rows // 2), "row")
    alignment_sensitivity = align_grad(
        alignment_tensor, gain, first_t, second_t, d_left, d_right
    )
    half = jnp.concatenate([summed(gathered[:, 0])[None], gathered[:, 1]], axis=0)
    half, alignment_sensitivity = lax.optimization_barrier((half, alignment_sensitivity))
    outs = unpack(
        core,
        half,
        from_partner(half),
        1.0 / amino_number,
        (
            final_mapping_matrix.shape,
            feedforward_expand_matrix.shape,
            feedforward_contract_matrix.shape,
            first_factor_matrix.shape[::-1],
            second_factor_matrix.shape[::-1],
        ),
    )
    return (result, grad, alignment_sensitivity, *outs[:3], outs[3].T, outs[4].T)


def solution(mesh):
    return jax.shard_map(
        on_device,
        mesh=mesh,
        in_specs=(
            P(None, ("row", "col"), None),
            P(),
            P(),
            P(),
            P(),
            P(),
            P("row", "col", None),
            P(),
            P(),
            P(),
            P("row", "col", None),
        ),
        out_specs=(
            P("row", "col", None),
            P("row", "col", None),
            P(None, ("row", "col"), None),
            P(),
            P(),
            P(),
            P(),
            P(),
        ),
        check_vma=False,
    )
```
